16 devices in a mesh: att: 4 (over z, y), emb: 4 (over x, core).
Axes of the slice: x: 2, y: 2, z: 2, core: 2. Of those that a mesh axis runs over, the one named last changes fastest.
Arguments:
- w_qkv: float32 [4, 3, 2048, 2048], P(None, None, 'emb', 'att')
- w_out: float32 [4, 2048, 2048], P(None, 'att', 'emb')
- x_in: bfloat16 [4, 2048, 2048], P(None, None, 'emb')
- dy_qkv: bfloat16 [4, 3, 2048, 2048], P(None, None, None, 'att')
- x_attn: bfloat16 [4, 2048, 2048], P(None, None, 'att')
- dy_out: bfloat16 [4, 2048, 2048], P(None, None, 'emb')
- r_qkv: float32 [4, 3, 2048], P(None, None, 'emb')
- c_qkv: float32 [4, 3, 2048], P(None, None, 'att')
- r_out: float32 [4, 2048], P(None, 'att')
- c_out: float32 [4, 2048], P(None, 'emb')
- hyper_params: float32 [3], replicated
Outputs:
- output 1: float32 [4, 3, 2048, 2048], P(None, None, 'emb', 'att')
- output 2: float32 [4, 2048, 2048], P(None, 'att', 'emb')
- output 3: float32 [4, 3, 2048], P(None, None, 'emb')
- output 4: float32 [4, 3, 2048], P(None, None, 'att')
- output 5: float32 [4, 2048], P(None, 'att')
- output 6: float32 [4, 2048], P(None, 'emb')
All inputs are finite; a program needn't handle non-finite values.
Results may differ from the reference program's by a relative error of at most 0.001.
Values are sent between devices in bfloat16 or wider.
A program may use at most 1 GiB of HBM per device.

```python
import functools
import jax
import jax.numpy as jnp
from jax import lax

D = 2048
HEADS = 16
HEAD = 128
TOKENS = 2048
LAYERS = 4

INNER = HEADS * HEAD
EPS_SQUARE = 1e-30
EPS_SCALE = 1e-3


def cos_scale(rng_key, lead_shape, length, amplitude):
    phase_off = jax.random.uniform(rng_key, lead_shape + (1,), jnp.float32)
    position = jnp.arange(length, dtype=jnp.float32) / length
    return jnp.exp(amplitude * jnp.cos(2.0 * jnp.pi * (position + phase_off)))


def scaled_tokens(rng_key, lead_shape, length, factor):
    key_noise, key_scale = jax.random.split(rng_key)
    gauss_noise = jax.random.normal(key_noise, lead_shape + (2, TOKENS // 2, length), jnp.float32)
    scales = cos_scale(key_scale, lead_shape + (2, 1), length, 0.75)
    return (gauss_noise * scales * factor).reshape(lead_shape + (TOKENS, length)).astype(jnp.bfloat16)


def scaled_weight(rng_key, lead_shape, n_rows, n_cols):
    key_noise, key_row, key_col = jax.random.split(rng_key, 3)
    gauss_noise = jax.random.normal(key_noise, lead_shape + (n_rows, n_cols), jnp.float32)
    row_scale = cos_scale(key_row, lead_shape, n_rows, 0.5)
    col_scale = cos_scale(key_col, lead_shape, n_cols, 0.5)
    return gauss_noise * row_scale[..., :, None] * col_scale[..., None, :] * n_rows ** -0.5


def setup_inputs(seed: int = 0) -> dict:
    key_list = jax.random.split(jax.random.key(seed), 11)
    tok_norm = TOKENS ** -0.5
    low_end = jnp.array([0.5, 0.5, 0.2], jnp.float32)
    high_end = jnp.array([0.8, 1.0, 0.4], jnp.float32)
    return {
        "w_qkv": scaled_weight(key_list[0], (LAYERS, 3), D, INNER),
        "w_out": scaled_weight(key_list[1], (LAYERS,), INNER, D),
        "x_in": scaled_tokens(key_list[2], (LAYERS,), D, 1.0),
        "dy_qkv": scaled_tokens(key_list[3], (LAYERS, 3), INNER, tok_norm),
        "x_attn": scaled_tokens(key_list[4], (LAYERS,), INNER, 1.0),
        "dy_out": scaled_tokens(key_list[5], (LAYERS,), D, tok_norm),
        "r_qkv": jax.random.uniform(key_list[6], (LAYERS, 3, D), jnp.float32, 0.2, 1.0),
        "c_qkv": jax.random.uniform(key_list[7], (LAYERS, 3, INNER), jnp.float32, 0.2, 1.0),
        "r_out": jax.random.uniform(key_list[8], (LAYERS, INNER), jnp.float32, 0.2, 1.0),
        "c_out": jax.random.uniform(key_list[9], (LAYERS, D), jnp.float32, 0.2, 1.0),
        "hyper_params": jax.random.uniform(key_list[10], (3,), jnp.float32, low_end, high_end),
    }


def adafactor_one(w_grad, weight, row_old, col_old, hyper_params):
    beta_two = hyper_params[0]
    rel_step = hyper_params[1]
    clip_limit = hyper_params[2]
    q_sq = w_grad * w_grad + EPS_SQUARE
    row_new = beta_two * row_old + (1.0 - beta_two) * jnp.mean(q_sq, axis=1)
    col_new = beta_two * col_old + (1.0 - beta_two) * jnp.mean(q_sq, axis=0)
    second = row_new[:, None] * col_new[None, :] / jnp.mean(row_new)
    update = w_grad / jnp.sqrt(second)
    rms_u = jnp.sqrt(jnp.mean(update * update))
    clipped = update / jnp.maximum(1.0, rms_u / clip_limit)
    step_size = rel_step * jnp.maximum(EPS_SCALE, jnp.sqrt(jnp.mean(weight * weight)))
    return weight - step_size * clipped, row_new, col_new


def reference(w_qkv, w_out, x_in, dy_qkv, x_attn, dy_out, r_qkv, c_qkv, r_out, c_out, hyper_params):
    step_fn = functools.partial(adafactor_one, hyper_params=hyper_params)

    def one_layer(carry, layer_in):
        lw_qkv, lw_out, lx_in, ldy_qkv, lx_attn, ldy_out, lr_qkv, lc_qkv, lr_out, lc_out = layer_in
        g_qkv = jnp.einsum("td,ktn->kdn", lx_in.astype(jnp.float32), ldy_qkv.astype(jnp.float32))
        g_out = jnp.dot(lx_attn.T, ldy_out, preferred_element_type=jnp.float32)
        new_qkv = jax.vmap(step_fn)(g_qkv, lw_qkv, lr_qkv, lc_qkv)
        new_out = step_fn(g_out, lw_out, lr_out, lc_out)
        return carry, (new_qkv[0], new_out[0], new_qkv[1], new_qkv[2], new_out[1], new_out[2])

    final_carry, results = lax.scan(
        one_layer,
        jnp.zeros((), jnp.float32),
        (w_qkv, w_out, x_in, dy_qkv, x_attn, dy_out, r_qkv, c_qkv, r_out, c_out),
    )
    return (results[0], results[1], results[2], results[3], results[4], results[5])
```

```python
import functools

import jax
import jax.numpy as jnp
from jax import lax
from jax.experimental import pallas as pl
from jax.experimental.pallas import tpu as pltpu
from jax.sharding import PartitionSpec as P

EPS_SQUARE = 1e-30
EPS_SCALE = 1e-3
MESH = pl.DeviceIdType.MESH
F32 = jnp.float32
BF16 = jnp.bfloat16
NA = 4
NE = 4
LAYERS = 4
MATS = 16
TOK = 2048
B = 512
LANES = 128
NDY = 5
NX = 3
KCH = 4
GROUPS = ((0, 4), (4, 4), (8, 4), (12, 2), (14, 1), (15, 1))


def col_of(row_piece):
    return jnp.broadcast_to(row_piece, (LANES, LANES)).T


def stats_body(
    n_total,
    w_qkv, w_out, x_in, dy_qkv, x_attn, dy_out, r_qkv, c_qkv, r_out, c_out, hyper,
    g, w, rq, cq, ro, co, bs,
    xbuf, dybuf, attbuf, embbuf, bbuf, rq_old, cq_old, ro_old, co_old, hp,
    xsem, dysem, wsem, insem, ch_sem, a_send, a_recv, e_send, e_recv, b_send, b_recv,
):
    a = lax.axis_index("att")
    e = lax.axis_index("emb")
    me = a * NE + e

    barrier = pltpu.get_barrier_semaphore()
    for da in range(NA):
        for de in range(NE):
            if da or de:
                pl.semaphore_signal(
                    barrier, inc=1, device_id=(lax.rem(a + da, NA), lax.rem(e + de, NE)), device_id_type=MESH
                )

    def x_copy(xi):
        l, kind = divmod(xi, 2)
        src = (x_attn if kind else x_in).at[l]
        return pltpu.make_async_copy(src, xbuf.at[xi % NX], xsem.at[xi % NX])

    def dy_copy(s):
        l, m = divmod(s, 4)
        src = dy_out.at[l] if m == 3 else dy_qkv.at[l, m]
        return pltpu.make_async_copy(src, dybuf.at[s % NDY], dysem.at[s % NDY])

    def w_copy(s):
        l, m = divmod(s, 4)
        src = w_out.at[l] if m == 3 else w_qkv.at[l, m]
        return pltpu.make_async_copy(src, w.at[s], wsem.at[s])

    def first_chunk(k):
        rows = pl.ds(k * (TOK // KCH), TOK // KCH)
        return (
            pltpu.make_async_copy(x_in.at[0, rows], xbuf.at[0, rows], ch_sem.at[2 * k]),
            pltpu.make_async_copy(dy_qkv.at[0, 0, rows], dybuf.at[0, rows], ch_sem.at[2 * k + 1]),
        )

    small = [
        pltpu.make_async_copy(r_qkv, rq_old, insem.at[0]),
        pltpu.make_async_copy(c_qkv, cq_old, insem.at[1]),
        pltpu.make_async_copy(r_out, ro_old, insem.at[2]),
        pltpu.make_async_copy(c_out, co_old, insem.at[3]),
        pltpu.make_async_copy(hyper, hp, insem.at[4]),
    ]

    for k in range(KCH):
        for c in first_chunk(k):
            c.start()
    dy_copy(1).start()
    dy_copy(2).start()
    for c in small:
        c.start()

    def stats(s):
        is_out = s % 4 == 3
        row_dst, row_me = (embbuf, e) if is_out else (attbuf, a)
        col_dst, col_me = (attbuf, a) if is_out else (embbuf, e)
        acc = [None] * 4
        for c in range(4):
            rows = pl.ds(c * LANES, LANES)
            lane_part = None
            for j in range(4):
                blk = g[s, rows, pl.ds(j * LANES, LANES)]
                sq = blk * blk
                lane_part = sq if lane_part is None else lane_part + sq
                part = jnp.sum(sq.reshape(LANES // 8, 8, LANES), axis=0)
                acc[j] = part if acc[j] is None else acc[j] + part
            row_dst[row_me, s, c : c + 1, :] = jnp.sum(lane_part.T, axis=0, keepdims=True)
        for j in range(4):
            col_dst[col_me, s, j : j + 1, :] = jnp.sum(acc[j], axis=0, keepdims=True)

    def a_copies(gi):
        s0, n = GROUPS[gi]
        sl = pl.ds(s0, n)
        out = []
        for d in range(1, NA):
            out.append(
                pltpu.make_async_remote_copy(
                    src_ref=attbuf.at[a, sl], dst_ref=attbuf.at[a, sl],
                    send_sem=a_send.at[gi, d], recv_sem=a_recv.at[gi, a],
                    device_id=(lax.rem(a + d, NA), e), device_id_type=MESH,
                )
            )
        for d in range(1, NE):
            out.append(
                pltpu.make_async_remote_copy(
                    src_ref=embbuf.at[e, sl], dst_ref=embbuf.at[e, sl],
                    send_sem=e_send.at[gi, d], recv_sem=e_recv.at[gi, e],
                    device_id=(a, lax.rem(e + d, NE)), device_id_type=MESH,
                )
            )
        return out

    def a_wait(gi):
        s0, n = GROUPS[gi]
        sl = pl.ds(s0, n)
        for d in range(1, NA):
            src = lax.rem(a + d, NA)
            pltpu.make_async_remote_copy(
                src_ref=attbuf.at[src, sl], dst_ref=attbuf.at[src, sl],
                send_sem=a_send.at[gi, d], recv_sem=a_recv.at[gi, src],
                device_id=(src, e), device_id_type=MESH,
            ).wait_recv()
        for d in range(1, NE):
            src = lax.rem(e + d, NE)
            pltpu.make_async_remote_copy(
                src_ref=embbuf.at[src, sl], dst_ref=embbuf.at[src, sl],
                send_sem=e_send.at[gi, d], recv_sem=e_recv.at[gi, src],
                device_id=(a, src), device_id_type=MESH,
            ).wait_recv()

    def b_copy(l, d, to):
        da, de = divmod(d, NE)
        if to:
            src = me
            dev = (lax.rem(a + da, NA), lax.rem(e + de, NE))
        else:
            dev = (lax.rem(a + da, NA), lax.rem(e + de, NE))
            src = dev[0] * NE + dev[1]
        return pltpu.make_async_remote_copy(
            src_ref=bbuf.at[l, src], dst_ref=bbuf.at[l, src],
            send_sem=b_send.at[l, d], recv_sem=b_recv.at[l, src],
            device_id=dev, device_id_type=MESH,
        )

    lane = lax.broadcasted_iota(jnp.int32, (1, LANES), 1)

    def finish(s):
        l, m = divmod(s, 4)
        is_out = m == 3
        row_src, col_src = (embbuf, attbuf) if is_out else (attbuf, embbuf)
        beta = hp[0]
        one_beta = 1.0 - beta
        acc = [None] * 4
        r_sum = None
        for c in range(4):
            ls = pl.ds(c * LANES, LANES)
            tot = (row_src[0, s, c : c + 1, :] + row_src[1, s, c : c + 1, :]) + (
                row_src[2, s, c : c + 1, :] + row_src[3, s, c : c + 1, :]
            )
            old = ro_old[l : l + 1, ls] if is_out else rq_old[m, l : l + 1, ls]
            r_new = beta * old + one_beta * (tot * (1.0 / n_total) + EPS_SQUARE)
            if is_out:
                ro[l : l + 1, ls] = r_new
            else:
                rq[m, l : l + 1, ls] = r_new
            r_sum = r_new if r_sum is None else r_sum + r_new
            factor = col_of(lax.rsqrt(r_new))
            for j in range(4):
                t = g[s, ls, pl.ds(j * LANES, LANES)] * factor
                part = jnp.sum((t * t).reshape(LANES // 8, 8, LANES), axis=0)
                acc[j] = part if acc[j] is None else acc[j] + part
        u = None
        for c in range(4):
            ls = pl.ds(c * LANES, LANES)
            tot = (col_src[0, s, c : c + 1, :] + col_src[1, s, c : c + 1, :]) + (
                col_src[2, s, c : c + 1, :] + col_src[3, s, c : c + 1, :]
            )
            old = co_old[l : l + 1, ls] if is_out else cq_old[m, l : l + 1, ls]
            c_new = beta * old + one_beta * (tot * (1.0 / n_total) + EPS_SQUARE)
            if is_out:
                co[l : l + 1, ls] = c_new
            else:
                cq[m, l : l + 1, ls] = c_new
            col_factor = lax.rsqrt(c_new)
            part = acc[c] * (col_factor * col_factor)
            u = part if u is None else u + part
        bbuf[l, me, m : m + 1, :] = jnp.sum(u, axis=0, keepdims=True)
        w_sum = wsq[s]
        bbuf[l, me, 4 + m : 5 + m, :] = jnp.where(
            lane < LANES // 2, w_sum + pltpu.roll(w_sum, LANES // 2, 1), r_sum + pltpu.roll(r_sum, LANES // 2, 1)
        )

    wsq = {}

    def w_square(s):
        w_copy(s).wait()
        acc = None
        for c in range(4):
            for j in range(4):
                blk = w[s, pl.ds(c * LANES, LANES), pl.ds(j * LANES, LANES)]
                part = jnp.sum((blk * blk).reshape(LANES // 8, 8, LANES), axis=0)
                acc = part if acc is None else acc + part
        wsq[s] = jnp.sum(acc, axis=0, keepdims=True)

    DN = (((0,), (0,)), ((), ()))
    for s in range(MATS):
        l, m = divmod(s, 4)
        xi = 2 * l + (m == 3)
        if s + 3 < MATS:
            nl, nm = divmod(s + 3, 4)
            if nm == 3 or nm == 0:
                x_copy(2 * nl + (nm == 3)).start()
            dy_copy(s + 3).start()
        w_copy(s).start()
        if s == 5:
            pl.semaphore_wait(barrier, NA * NE - 1)
        for gi, (s0, n) in enumerate(GROUPS):
            if s0 + n + 1 == s:
                for c in a_copies(gi):
                    c.start()
        todo = []
        if s == 1:
            for c in small:
                c.wait()
        if s in (7, 11, 15):
            a_wait((s - 7) // 4)
            todo = [s - 7, s - 6]
        if s in (8, 12):
            todo = [s - 6, s - 5]
        if s in (9, 13):
            for d in range(1, NA * NE):
                b_copy((s - 9) // 4, d, True).start()
        if s >= 2:
            w_copy_todo = [s - 2]
        else:
            w_copy_todo = []
        if s == 0:
            for k in range(KCH):
                rows = pl.ds(k * (TOK // KCH), TOK // KCH)
                for c in first_chunk(k):
                    c.wait()
                part = lax.dot_general(xbuf[0, rows], dybuf[0, rows], DN, preferred_element_type=F32)
                g[0] = part if k == 0 else g[0] + part
        else:
            if m == 0 or m == 3:
                x_copy(xi).wait()
            dy_copy(s).wait()
            g[s] = lax.dot_general(xbuf[xi % NX], dybuf[s % NDY], DN, preferred_element_type=F32)
        if s >= 1:
            stats(s - 1)
        for t in w_copy_todo:
            w_square(t)
        for t in todo:
            finish(t)

    for c in a_copies(4):
        c.start()
    stats(15)
    for c in a_copies(5):
        c.start()
    w_square(14)
    w_square(15)
    finish(10)
    finish(11)
    for d in range(1, NA * NE):
        b_copy(2, d, True).start()
    a_wait(3)
    finish(12)
    finish(13)
    a_wait(4)
    finish(14)
    a_wait(5)
    finish(15)
    for d in range(1, NA * NE):
        b_copy(3, d, True).start()
    for l in range(LAYERS):
        for d in range(1, NA * NE):
            b_copy(l, d, False).wait_recv()
        tot = bbuf[l, 0]
        for d in range(1, NA * NE):
            tot = tot + bbuf[l, d]
        bs[l] = tot
    for gi in range(len(GROUPS)):
        for c in a_copies(gi):
            c.wait_send()
    for l in range(LAYERS):
        for d in range(1, NA * NE):
            b_copy(l, d, True).wait_send()


NOUT = 4


def update_body(
    n_total, g, w, rq, cq, ro, co, bs, hyper,
    w_qkv_new, w_out_new, rq_new, cq_new, ro_new, co_new,
    obuf, hp, osem, rsem, hsem,
):
    load_hp = pltpu.make_async_copy(hyper, hp, hsem)
    load_hp.start()
    small = [
        pltpu.make_async_copy(rq, rq_new, rsem.at[0]),
        pltpu.make_async_copy(cq, cq_new, rsem.at[1]),
        pltpu.make_async_copy(ro, ro_new, rsem.at[2]),
        pltpu.make_async_copy(co, co_new, rsem.at[3]),
    ]
    for c in small:
        c.start()
    load_hp.wait()
    rho = hp[1]
    clip = hp[2]
    n_elems = float(n_total) * float(n_total)
    lane = lax.broadcasted_iota(jnp.int32, (1, LANES), 1)
    low = lane < LANES // 2

    def out_copy(s):
        l, m = divmod(s, 4)
        dst = w_out_new.at[l] if m == 3 else w_qkv_new.at[l, m]
        return pltpu.make_async_copy(obuf.at[s % NOUT], dst, osem.at[s % NOUT])

    for l in range(LAYERS):
        u_sum = jnp.sum(bs[l, 0:4, :], axis=1, keepdims=True)
        wr = bs[l, 4:8, :]
        w_sum = jnp.sum(jnp.where(low, wr, 0.0), axis=1, keepdims=True)
        r_mean = jnp.sum(jnp.where(low, 0.0, wr), axis=1, keepdims=True) * (0.25 / n_total)
        rms_u = jnp.sqrt(u_sum * r_mean / n_elems)
        rms_w = jnp.sqrt(w_sum / n_elems)
        step = rho * jnp.maximum(EPS_SCALE, rms_w) * jnp.sqrt(r_mean) / jnp.maximum(1.0, rms_u / clip)
        for m in range(4):
            s = 4 * l + m
            if s >= NOUT:
                out_copy(s - NOUT).wait()
            st = step[m : m + 1, :]
            cols = []
            for j in range(4):
                ls = pl.ds(j * LANES, LANES)
                c_new = co[l : l + 1, ls] if m == 3 else cq[m, l : l + 1, ls]
                cols.append(lax.rsqrt(c_new) * st)
            for c in range(4):
                ls = pl.ds(c * LANES, LANES)
                r_new = ro[l : l + 1, ls] if m == 3 else rq[m, l : l + 1, ls]
                factor = col_of(lax.rsqrt(r_new))
                for j in range(4):
                    js = pl.ds(j * LANES, LANES)
                    obuf[s % NOUT, ls, js] = w[s, ls, js] - (g[s, ls, js] * factor) * cols[j]
            out_copy(s).start()
    for s in range(MATS - NOUT, MATS):
        out_copy(s).wait()
    for c in small:
        c.wait()


def solution(mesh):
    in_specs = (
        P(None, None, "emb", "att"),
        P(None, "att", "emb"),
        P(None, None, "emb"),
        P(None, None, None, "att"),
        P(None, None, "att"),
        P(None, None, "emb"),
        P(None, None, "emb"),
        P(None, None, "att"),
        P(None, "att"),
        P(None, "emb"),
        P(),
    )
    out_specs = (
        P(None, None, "emb", "att"),
        P(None, "att", "emb"),
        P(None, None, "emb"),
        P(None, None, "att"),
        P(None, "att"),
        P(None, "emb"),
    )
    n_total = B * NA
    hbm = pl.BlockSpec(memory_space=pltpu.HBM)
    vm = pl.BlockSpec(memory_space=pltpu.VMEM)
    dma = pltpu.SemaphoreType.DMA

    def local_run(w_qkv, w_out, x_in, dy_qkv, x_attn, dy_out, r_qkv, c_qkv, r_out, c_out, hyper_params):
        ng = len(GROUPS)
        swap = lambda v: jnp.transpose(v, (1, 0, 2))
        mid = pl.pallas_call(
            functools.partial(stats_body, n_total),
            out_shape=(
                pltpu.VMEM((MATS, B, B), F32),
                pltpu.VMEM((MATS, B, B), F32),
                pltpu.VMEM((3, LAYERS, B), F32),
                pltpu.VMEM((3, LAYERS, B), F32),
                pltpu.VMEM((LAYERS, B), F32),
                pltpu.VMEM((LAYERS, B), F32),
                pltpu.VMEM((LAYERS, 8, LANES), F32),
            ),
            in_specs=[hbm] * 11,
            out_specs=(vm,) * 7,
            scratch_shapes=[
                pltpu.VMEM((NX, TOK, B), BF16),
                pltpu.VMEM((NDY, TOK, B), BF16),
                pltpu.VMEM((NA, MATS, 4, LANES), F32),
                pltpu.VMEM((NE, MATS, 4, LANES), F32),
                pltpu.VMEM((LAYERS, NA * NE, 8, LANES), F32),
                pltpu.VMEM((3, LAYERS, B), F32),
                pltpu.VMEM((3, LAYERS, B), F32),
                pltpu.VMEM((LAYERS, B), F32),
                pltpu.VMEM((LAYERS, B), F32),
                pltpu.SMEM((3,), F32),
                dma((NX,)),
                dma((NDY,)),
                dma((MATS,)),
                dma((5,)),
                dma((2 * KCH,)),
                dma((ng, NA)),
                dma((ng, NA)),
                dma((ng, NE)),
                dma((ng, NE)),
                dma((LAYERS, NA * NE)),
                dma((LAYERS, NA * NE)),
            ],
            compiler_params=pltpu.CompilerParams(
                collective_id=0, has_side_effects=True, vmem_limit_bytes=24 * 2**20
            ),
            name="stats",
        )(w_qkv, w_out, x_in, dy_qkv, x_attn, dy_out, swap(r_qkv), swap(c_qkv), r_out, c_out, hyper_params)
        new = pl.pallas_call(
            functools.partial(update_body, n_total),
            out_shape=(
                jax.ShapeDtypeStruct(w_qkv.shape, F32),
                jax.ShapeDtypeStruct(w_out.shape, F32),
                jax.ShapeDtypeStruct((3, LAYERS, B), F32),
                jax.ShapeDtypeStruct((3, LAYERS, B), F32),
                jax.ShapeDtypeStruct(r_out.shape, F32),
                jax.ShapeDtypeStruct(c_out.shape, F32),
            ),
            in_specs=[vm] * 7 + [hbm],
            out_specs=(hbm,) * 6,
            scratch_shapes=[
                pltpu.VMEM((NOUT, B, B), F32),
                pltpu.SMEM((3,), F32),
                dma((NOUT,)),
                dma((4,)),
                dma,
            ],
            compiler_params=pltpu.CompilerParams(vmem_limit_bytes=8 * 2**20),
            name="update",
        )(*mid, hyper_params)
        return new[0], new[1], swap(new[2]), swap(new[3]), new[4], new[5]

    return jax.shard_map(local_run, mesh=mesh, in_specs=in_specs, out_specs=out_specs, check_vma=False)
```

```python
import functools

import jax
import jax.numpy as jnp
from jax import lax
from jax.experimental import pallas as pl
from jax.experimental.pallas import tpu as pltpu
from jax.sharding import PartitionSpec as P

EPS_SQUARE = 1e-30
EPS_SCALE = 1e-3
MESH = pl.DeviceIdType.MESH
F32 = jnp.float32
BF16 = jnp.bfloat16
NA = 4
NE = 4
LAYERS = 4
MATS = 16
TOK = 2048
B = 512
LANES = 128
NDY = 5
NX = 3
KCH = 4
LAST = 12
NG = 12
GROUPS = ((0, 4), (4, 4), (8, 4), (12, 2), (14, 1), (15, 1))


A_WAIT = {7: 0, 11: 1, 15: 2}
B_SEND = {9: 0, 13: 1}
FINISHES = {0: 7, 1: 7, 2: 8, 3: 8, 4: 11, 5: 11, 6: 12, 7: 12, 8: 15, 9: 15, 10: 15, 11: 15}
UPDATES = {0: 11, 1: 12, 2: 13, 3: 13, 4: 15, 5: 15, 6: 15, 7: 15}


def col_of(row_piece):
    return jnp.broadcast_to(row_piece, (LANES, LANES)).T


def step_sizes(tot, n_total, rho, clip):
    n_elems = float(n_total) * float(n_total)
    low = lax.broadcasted_iota(jnp.int32, (1, LANES), 1) < LANES // 2
    u_sum = jnp.sum(tot[0:4, :], axis=1, keepdims=True)
    w_sum = jnp.sum(jnp.where(low, tot[4:8, :], 0.0), axis=1, keepdims=True)
    r_mean = jnp.sum(jnp.where(low, 0.0, tot[4:8, :]), axis=1, keepdims=True) * (0.25 / n_total)
    rms_u = jnp.sqrt(u_sum * r_mean / n_elems)
    rms_w = jnp.sqrt(w_sum / n_elems)
    return rho * jnp.maximum(EPS_SCALE, rms_w) * jnp.sqrt(r_mean) / jnp.maximum(1.0, rms_u / clip)


def update_one(dst, w_ref, g_ref, row_pieces, col_pieces, st):
    cols = [lax.rsqrt(c_new) * st for c_new in col_pieces]
    for c in range(4):
        ls = pl.ds(c * LANES, LANES)
        factor = col_of(lax.rsqrt(row_pieces[c]))
        for j in range(4):
            js = pl.ds(j * LANES, LANES)
            dst[ls, js] = w_ref[ls, js] - (g_ref[ls, js] * factor) * cols[j]


def stats_body(
    n_total,
    w_qkv, w_out, x_in, dy_qkv, x_attn, dy_out, r_qkv, c_qkv, r_out, c_out, hyper,
    wn, g3, w3, rq, cq, ro, co, bs,
    xbuf, dybuf, attbuf, embbuf, bbuf, rq_old, cq_old, ro_old, co_old, hp, gring,
    xsem, dysem, wsem, insem, ch_sem, a_send, a_recv, e_send, e_recv, b_send, b_recv,
):
    a = lax.axis_index("att")
    e = lax.axis_index("emb")
    me = a * NE + e

    barrier = pltpu.get_barrier_semaphore()
    for da in range(NA):
        for de in range(NE):
            if da or de:
                pl.semaphore_signal(
                    barrier, inc=1, device_id=(lax.rem(a + da, NA), lax.rem(e + de, NE)), device_id_type=MESH
                )

    def g_at(s):
        return g3.at[s - LAST] if s >= LAST else gring.at[s % NG]

    def w_at(s):
        return w3.at[s - LAST] if s >= LAST else wn.at[s]

    def x_copy(xi):
        l, kind = divmod(xi, 2)
        src = (x_attn if kind else x_in).at[l]
        return pltpu.make_async_copy(src, xbuf.at[xi % NX], xsem.at[xi % NX])

    def dy_copy(s):
        l, m = divmod(s, 4)
        src = dy_out.at[l] if m == 3 else dy_qkv.at[l, m]
        return pltpu.make_async_copy(src, dybuf.at[s % NDY], dysem.at[s % NDY])

    def w_copy(s):
        l, m = divmod(s, 4)
        src = w_out.at[l] if m == 3 else w_qkv.at[l, m]
        return pltpu.make_async_copy(src, w_at(s), wsem.at[s])

    def first_chunk(k):
        rows = pl.ds(k * (TOK // KCH), TOK // KCH)
        return (
            pltpu.make_async_copy(x_in.at[0, rows], xbuf.at[0, rows], ch_sem.at[2 * k]),
            pltpu.make_async_copy(dy_qkv.at[0, 0, rows], dybuf.at[0, rows], ch_sem.at[2 * k + 1]),
        )

    small = [
        pltpu.make_async_copy(r_qkv, rq_old, insem.at[0]),
        pltpu.make_async_copy(c_qkv, cq_old, insem.at[1]),
        pltpu.make_async_copy(r_out, ro_old, insem.at[2]),
        pltpu.make_async_copy(c_out, co_old, insem.at[3]),
        pltpu.make_async_copy(hyper, hp, insem.at[4]),
    ]

    for k in range(KCH):
        for c in first_chunk(k):
            c.start()
    dy_copy(1).start()
    dy_copy(2).start()
    for c in small:
        c.start()

    def stats(s):
        is_out = s % 4 == 3
        row_dst, row_me = (embbuf, e) if is_out else (attbuf, a)
        col_dst, col_me = (attbuf, a) if is_out else (embbuf, e)
        acc = [None] * 4
        for c in range(4):
            rows = pl.ds(c * LANES, LANES)
            lane_part = None
            for j in range(4):
                blk = g_at(s)[rows, pl.ds(j * LANES, LANES)]
                sq = blk * blk
                lane_part = sq if lane_part is None else lane_part + sq
                part = jnp.sum(sq.reshape(LANES // 8, 8, LANES), axis=0)
                acc[j] = part if acc[j] is None else acc[j] + part
            row_dst[row_me, s, c : c + 1, :] = jnp.sum(lane_part.T, axis=0, keepdims=True)
        for j in range(4):
            col_dst[col_me, s, j : j + 1, :] = jnp.sum(acc[j], axis=0, keepdims=True)

    def a_copies(gi):
        s0, n = GROUPS[gi]
        sl = pl.ds(s0, n)
        out = []
        for d in range(1, NA):
            out.append(
                pltpu.make_async_remote_copy(
                    src_ref=attbuf.at[a, sl], dst_ref=attbuf.at[a, sl],
                    send_sem=a_send.at[gi, d], recv_sem=a_recv.at[gi, a],
                    device_id=(lax.rem(a + d, NA), e), device_id_type=MESH,
                )
            )
        for d in range(1, NE):
            out.append(
                pltpu.make_async_remote_copy(
                    src_ref=embbuf.at[e, sl], dst_ref=embbuf.at[e, sl],
                    send_sem=e_send.at[gi, d], recv_sem=e_recv.at[gi, e],
                    device_id=(a, lax.rem(e + d, NE)), device_id_type=MESH,
                )
            )
        return out

    def a_wait(gi):
        s0, n = GROUPS[gi]
        sl = pl.ds(s0, n)
        for d in range(1, NA):
            src = lax.rem(a + d, NA)
            pltpu.make_async_remote_copy(
                src_ref=attbuf.at[src, sl], dst_ref=attbuf.at[src, sl],
                send_sem=a_send.at[gi, d], recv_sem=a_recv.at[gi, src],
                device_id=(src, e), device_id_type=MESH,
            ).wait_recv()
        for d in range(1, NE):
            src = lax.rem(e + d, NE)
            pltpu.make_async_remote_copy(
                src_ref=embbuf.at[src, sl], dst_ref=embbuf.at[src, sl],
                send_sem=e_send.at[gi, d], recv_sem=e_recv.at[gi, src],
                device_id=(a, src), device_id_type=MESH,
            ).wait_recv()

    def b_copy(l, d, to):
        da, de = divmod(d, NE)
        if to:
            src = me
            dev = (lax.rem(a + da, NA), lax.rem(e + de, NE))
        else:
            dev = (lax.rem(a + da, NA), lax.rem(e + de, NE))
            src = dev[0] * NE + dev[1]
        return pltpu.make_async_remote_copy(
            src_ref=bbuf.at[l, src], dst_ref=bbuf.at[l, src],
            send_sem=b_send.at[l, d], recv_sem=b_recv.at[l, src],
            device_id=dev, device_id_type=MESH,
        )

    lane = lax.broadcasted_iota(jnp.int32, (1, LANES), 1)

    def finish(s):
        l, m = divmod(s, 4)
        is_out = m == 3
        row_src, col_src = (embbuf, attbuf) if is_out else (attbuf, embbuf)
        beta = hp[0]
        one_beta = 1.0 - beta
        acc = [None] * 4
        r_sum = None
        for c in range(4):
            ls = pl.ds(c * LANES, LANES)
            tot = (row_src[0, s, c : c + 1, :] + row_src[1, s, c : c + 1, :]) + (
                row_src[2, s, c : c + 1, :] + row_src[3, s, c : c + 1, :]
            )
            old = ro_old[l : l + 1, ls] if is_out else rq_old[m, l : l + 1, ls]
            r_new = beta * old + one_beta * (tot * (1.0 / n_total) + EPS_SQUARE)
            if is_out:
                ro[l : l + 1, ls] = r_new
            else:
                rq[m, l : l + 1, ls] = r_new
            r_sum = r_new if r_sum is None else r_sum + r_new
            factor = col_of(lax.rsqrt(r_new))
            for j in range(4):
                t = g_at(s)[ls, pl.ds(j * LANES, LANES)] * factor
                part = jnp.sum((t * t).reshape(LANES // 8, 8, LANES), axis=0)
                acc[j] = part if acc[j] is None else acc[j] + part
        u = None
        for c in range(4):
            ls = pl.ds(c * LANES, LANES)
            tot = (col_src[0, s, c : c + 1, :] + col_src[1, s, c : c + 1, :]) + (
                col_src[2, s, c : c + 1, :] + col_src[3, s, c : c + 1, :]
            )
            old = co_old[l : l + 1, ls] if is_out else cq_old[m, l : l + 1, ls]
            c_new = beta * old + one_beta * (tot * (1.0 / n_total) + EPS_SQUARE)
            if is_out:
                co[l : l + 1, ls] = c_new
            else:
                cq[m, l : l + 1, ls] = c_new
            col_factor = lax.rsqrt(c_new)
            part = acc[c] * (col_factor * col_factor)
            u = part if u is None else u + part
        bbuf[l, me, m : m + 1, :] = jnp.sum(u, axis=0, keepdims=True)
        w_sum = wsq[s]
        bbuf[l, me, 4 + m : 5 + m, :] = jnp.where(
            lane < LANES // 2, w_sum + pltpu.roll(w_sum, LANES // 2, 1), r_sum + pltpu.roll(r_sum, LANES // 2, 1)
        )

    def pieces(s):
        l, m = divmod(s, 4)
        sl = [pl.ds(c * LANES, LANES) for c in range(4)]
        if m == 3:
            return [ro[l : l + 1, i] for i in sl], [co[l : l + 1, i] for i in sl]
        return [rq[m, l : l + 1, i] for i in sl], [cq[m, l : l + 1, i] for i in sl]

    steps = {}

    def gather_b(l):
        for d in range(1, NA * NE):
            b_copy(l, d, False).wait_recv()
        tot = bbuf[l, 0]
        for d in range(1, NA * NE):
            tot = tot + bbuf[l, d]
        return tot

    def update(s):
        l, m = divmod(s, 4)
        if l not in steps:
            steps[l] = step_sizes(gather_b(l), n_total, hp[1], hp[2])
        rows, cols = pieces(s)
        update_one(wn.at[s], wn.at[s], g_at(s), rows, cols, steps[l][m : m + 1, :])

    wsq = {}

    def w_square(s):
        w_copy(s).wait()
        acc = None
        for c in range(4):
            for j in range(4):
                blk = w_at(s)[pl.ds(c * LANES, LANES), pl.ds(j * LANES, LANES)]
                part = jnp.sum((blk * blk).reshape(LANES // 8, 8, LANES), axis=0)
                acc = part if acc is None else acc + part
        wsq[s] = jnp.sum(acc, axis=0, keepdims=True)

    DN = (((0,), (0,)), ((), ()))
    for s in range(MATS):
        l, m = divmod(s, 4)
        xi = 2 * l + (m == 3)
        if s + 3 < MATS:
            nl, nm = divmod(s + 3, 4)
            if nm == 3 or nm == 0:
                x_copy(2 * nl + (nm == 3)).start()
            dy_copy(s + 3).start()
        w_copy(s).start()
        if s == 5:
            pl.semaphore_wait(barrier, NA * NE - 1)
        for gi, (s0, n) in enumerate(GROUPS):
            if s0 + n + 1 == s:
                for c in a_copies(gi):
                    c.start()
        if s == 1:
            for c in small:
                c.wait()
        if s in A_WAIT:
            a_wait(A_WAIT[s])
        if s in B_SEND:
            for d in range(1, NA * NE):
                b_copy(B_SEND[s], d, True).start()
        ups = [t for t, at in UPDATES.items() if at == s]
        if ups and ups[0] // 4 not in steps:
            steps[ups[0] // 4] = step_sizes(gather_b(ups[0] // 4), n_total, hp[1], hp[2])
        if s == 0:
            for k in range(KCH):
                rows = pl.ds(k * (TOK // KCH), TOK // KCH)
                for c in first_chunk(k):
                    c.wait()
                part = lax.dot_general(xbuf[0, rows], dybuf[0, rows], DN, preferred_element_type=F32)
                g_at(0)[...] = part if k == 0 else g_at(0)[...] + part
        else:
            if m == 0 or m == 3:
                x_copy(xi).wait()
            dy_copy(s).wait()
            g_at(s)[...] = lax.dot_general(xbuf[xi % NX], dybuf[s % NDY], DN, preferred_element_type=F32)
        if s >= 1:
            stats(s - 1)
        if s >= 2:
            w_square(s - 2)
        for t, at in FINISHES.items():
            if at == s:
                finish(t)
        for t in ups:
            update(t)

    for c in a_copies(4):
        c.start()
    stats(15)
    for c in a_copies(5):
        c.start()
    for d in range(1, NA * NE):
        b_copy(2, d, True).start()
    w_square(14)
    w_square(15)
    a_wait(3)
    finish(12)
    finish(13)
    a_wait(4)
    finish(14)
    a_wait(5)
    finish(15)
    for d in range(1, NA * NE):
        b_copy(3, d, True).start()
    for t in (8, 9, 10, 11):
        update(t)
    bs[...] = gather_b(3)
    for gi in range(len(GROUPS)):
        for c in a_copies(gi):
            c.wait_send()
    for l in range(LAYERS):
        for d in range(1, NA * NE):
            b_copy(l, d, True).wait_send()


def update_body(
    n_total, wn, g3, w3, rq, cq, ro, co, bs, hyper,
    w_qkv_new, w_out_new, rq_new, cq_new, ro_new, co_new,
    obuf, hp, osem, rsem, hsem,
):
    load_hp = pltpu.make_async_copy(hyper, hp, hsem)
    load_hp.start()

    def out_copy(s):
        l, m = divmod(s, 4)
        dst = w_out_new.at[l] if m == 3 else w_qkv_new.at[l, m]
        return pltpu.make_async_copy(obuf.at[s - LAST] if s >= LAST else wn.at[s], dst, osem.at[s])

    for s in range(LAST):
        out_copy(s).start()
    small = [
        pltpu.make_async_copy(rq, rq_new, rsem.at[0]),
        pltpu.make_async_copy(cq, cq_new, rsem.at[1]),
        pltpu.make_async_copy(ro, ro_new, rsem.at[2]),
        pltpu.make_async_copy(co, co_new, rsem.at[3]),
    ]
    for c in small:
        c.start()
    load_hp.wait()
    l = LAYERS - 1
    step = step_sizes(bs[...], n_total, hp[1], hp[2])
    sl = [pl.ds(c * LANES, LANES) for c in range(4)]
    for m in range(4):
        if m == 3:
            rows, cols = [ro[l : l + 1, i] for i in sl], [co[l : l + 1, i] for i in sl]
        else:
            rows, cols = [rq[m, l : l + 1, i] for i in sl], [cq[m, l : l + 1, i] for i in sl]
        update_one(obuf.at[m], w3.at[m], g3.at[m], rows, cols, step[m : m + 1, :])
        out_copy(LAST + m).start()
    for s in range(MATS):
        out_copy(s).wait()
    for c in small:
        c.wait()


def solution(mesh):
    in_specs = (
        P(None, None, "emb", "att"),
        P(None, "att", "emb"),
        P(None, None, "emb"),
        P(None, None, None, "att"),
        P(None, None, "att"),
        P(None, None, "emb"),
        P(None, None, "emb"),
        P(None, None, "att"),
        P(None, "att"),
        P(None, "emb"),
        P(),
    )
    out_specs = (
        P(None, None, "emb", "att"),
        P(None, "att", "emb"),
        P(None, None, "emb"),
        P(None, None, "att"),
        P(None, "att"),
        P(None, "emb"),
    )
    n_total = B * NA
    hbm = pl.BlockSpec(memory_space=pltpu.HBM)
    vm = pl.BlockSpec(memory_space=pltpu.VMEM)
    dma = pltpu.SemaphoreType.DMA

    def local_run(w_qkv, w_out, x_in, dy_qkv, x_attn, dy_out, r_qkv, c_qkv, r_out, c_out, hyper_params):
        ng = len(GROUPS)
        swap = lambda v: jnp.transpose(v, (1, 0, 2))
        mid = pl.pallas_call(
            functools.partial(stats_body, n_total),
            out_shape=(
                pltpu.VMEM((LAST, B, B), F32),
                pltpu.VMEM((4, B, B), F32),
                pltpu.VMEM((4, B, B), F32),
                pltpu.VMEM((3, LAYERS, B), F32),
                pltpu.VMEM((3, LAYERS, B), F32),
                pltpu.VMEM((LAYERS, B), F32),
                pltpu.VMEM((LAYERS, B), F32),
                pltpu.VMEM((8, LANES), F32),
            ),
            in_specs=[hbm] * 11,
            out_specs=(vm,) * 8,
            scratch_shapes=[
                pltpu.VMEM((NX, TOK, B), BF16),
                pltpu.VMEM((NDY, TOK, B), BF16),
                pltpu.VMEM((NA, MATS, 4, LANES), F32),
                pltpu.VMEM((NE, MATS, 4, LANES), F32),
                pltpu.VMEM((LAYERS, NA * NE, 8, LANES), F32),
                pltpu.VMEM((3, LAYERS, B), F32),
                pltpu.VMEM((3, LAYERS, B), F32),
                pltpu.VMEM((LAYERS, B), F32),
                pltpu.VMEM((LAYERS, B), F32),
                pltpu.SMEM((3,), F32),
                pltpu.VMEM((NG, B, B), F32),
                dma((NX,)),
                dma((NDY,)),
                dma((MATS,)),
                dma((5,)),
                dma((2 * KCH,)),
                dma((ng, NA)),
                dma((ng, NA)),
                dma((ng, NE)),
                dma((ng, NE)),
                dma((LAYERS, NA * NE)),
                dma((LAYERS, NA * NE)),
            ],
            compiler_params=pltpu.CompilerParams(
                collective_id=0, has_side_effects=True, vmem_limit_bytes=36 * 2**20
            ),
            name="stats",
        )(w_qkv, w_out, x_in, dy_qkv, x_attn, dy_out, swap(r_qkv), swap(c_qkv), r_out, c_out, hyper_params)
        new = pl.pallas_call(
            functools.partial(update_body, n_total),
            out_shape=(
                jax.ShapeDtypeStruct(w_qkv.shape, F32),
                jax.ShapeDtypeStruct(w_out.shape, F32),
                jax.ShapeDtypeStruct((3, LAYERS, B), F32),
                jax.ShapeDtypeStruct((3, LAYERS, B), F32),
                jax.ShapeDtypeStruct(r_out.shape, F32),
                jax.ShapeDtypeStruct(c_out.shape, F32),
            ),
            in_specs=[vm] * 8 + [hbm],
            out_specs=(hbm,) * 6,
            scratch_shapes=[
                pltpu.VMEM((4, B, B), F32),
                pltpu.SMEM((3,), F32),
                dma((MATS,)),
                dma((4,)),
                dma,
            ],
            compiler_params=pltpu.CompilerParams(vmem_limit_bytes=6 * 2**20),
            name="update",
        )(*mid, hyper_params)
        return new[0], new[1], swap(new[2]), swap(new[3]), new[4], new[5]

    return jax.shard_map(local_run, mesh=mesh, in_specs=in_specs, out_specs=out_specs, check_vma=False)
```

```python
import functools

import jax
import jax.numpy as jnp
from jax import lax
from jax.experimental import pallas as pl
from jax.experimental.pallas import tpu as pltpu
from jax.sharding import PartitionSpec as P

EPS_SQUARE = 1e-30
EPS_SCALE = 1e-3
MESH = pl.DeviceIdType.MESH
F32 = jnp.float32
BF16 = jnp.bfloat16
NA = 4
NE = 4
LAYERS = 4
MATS = 16
TOK = 2048
B = 512
LANES = 128
NDY = 5
NX = 3
NW = 4
KCH = 4
LAST = 12
NG = 12
GROUPS = ((0, 4), (4, 4), (8, 4), (12, 2), (14, 1), (15, 1))


A_WAIT = {8: 0, 12: 1}
B_SEND = {12: 0}
FINISHES = {t: t + 8 for t in range(8)}


def col_of(row_piece):
    return jnp.broadcast_to(row_piece, (LANES, LANES)).T


def step_sizes(tot, n_total, rho, clip):
    n_elems = float(n_total) * float(n_total)
    low = lax.broadcasted_iota(jnp.int32, (1, LANES), 1) < LANES // 2
    u_sum = jnp.sum(tot[0:4, :], axis=1, keepdims=True)
    w_sum = jnp.sum(jnp.where(low, tot[4:8, :], 0.0), axis=1, keepdims=True)
    r_mean = jnp.sum(jnp.where(low, 0.0, tot[4:8, :]), axis=1, keepdims=True) * (0.25 / n_total)
    rms_u = jnp.sqrt(u_sum * r_mean / n_elems)
    rms_w = jnp.sqrt(w_sum / n_elems)
    return rho * jnp.maximum(EPS_SCALE, rms_w) * jnp.sqrt(r_mean) / jnp.maximum(1.0, rms_u / clip)


def update_one(dst, w_ref, g_ref, row_pieces, col_pieces, st):
    cols = [lax.rsqrt(c_new) * st for c_new in col_pieces]
    for c in range(4):
        ls = pl.ds(c * LANES, LANES)
        factor = col_of(lax.rsqrt(row_pieces[c]))
        for j in range(4):
            js = pl.ds(j * LANES, LANES)
            dst[ls, js] = w_ref[ls, js] - (g_ref[ls, js] * factor) * cols[j]


def stats_body(
    n_total,
    w_qkv, w_out, x_in, dy_qkv, x_attn, dy_out, r_qkv, c_qkv, r_out, c_out, hyper,
    wn, g3, w3, rq, cq, ro, co, bs,
    xbuf, dybuf, attbuf, embbuf, bbuf, rq_old, cq_old, ro_old, co_old, hp, gring,
    xsem, dysem, wsem, insem, ch_sem, send_sem, a_recv, e_recv, b_recv,
):
    a = lax.axis_index("att")
    e = lax.axis_index("emb")
    me = a * NE + e

    barrier = pltpu.get_barrier_semaphore()
    for da in range(NA):
        for de in range(NE):
            if da or de:
                pl.semaphore_signal(
                    barrier, inc=1, device_id=(lax.rem(a + da, NA), lax.rem(e + de, NE)), device_id_type=MESH
                )

    def g_at(s):
        return g3.at[s - LAST] if s >= LAST else gring.at[s % NG]

    def w_at(s):
        return w3.at[s - LAST] if s >= LAST else wn.at[s]

    def x_copy(xi):
        l, kind = divmod(xi, 2)
        src = (x_attn if kind else x_in).at[l]
        return pltpu.make_async_copy(src, xbuf.at[xi % NX], xsem.at[xi % NX])

    def dy_copy(s):
        l, m = divmod(s, 4)
        src = dy_out.at[l] if m == 3 else dy_qkv.at[l, m]
        return pltpu.make_async_copy(src, dybuf.at[s % NDY], dysem.at[s % NDY])

    def w_copy(s):
        l, m = divmod(s, 4)
        src = w_out.at[l] if m == 3 else w_qkv.at[l, m]
        return pltpu.make_async_copy(src, w_at(s), wsem.at[s % NW])

    def first_chunk(k):
        rows = pl.ds(k * (TOK // KCH), TOK // KCH)
        return (
            pltpu.make_async_copy(x_in.at[0, rows], xbuf.at[0, rows], ch_sem.at[2 * k]),
            pltpu.make_async_copy(dy_qkv.at[0, 0, rows], dybuf.at[0, rows], ch_sem.at[2 * k + 1]),
        )

    small = [
        pltpu.make_async_copy(r_qkv, rq_old, insem.at[0]),
        pltpu.make_async_copy(c_qkv, cq_old, insem.at[1]),
        pltpu.make_async_copy(r_out, ro_old, insem.at[2]),
        pltpu.make_async_copy(c_out, co_old, insem.at[3]),
        pltpu.make_async_copy(hyper, hp, insem.at[4]),
    ]

    for k in range(KCH):
        for c in first_chunk(k):
            c.start()
    dy_copy(1).start()
    dy_copy(2).start()
    for c in small:
        c.start()

    def stats(s):
        is_out = s % 4 == 3
        row_dst, row_me = (embbuf, e) if is_out else (attbuf, a)
        col_dst, col_me = (attbuf, a) if is_out else (embbuf, e)
        acc = [None] * 4
        for c in range(4):
            rows = pl.ds(c * LANES, LANES)
            lane_part = None
            for j in range(4):
                blk = g_at(s)[rows, pl.ds(j * LANES, LANES)]
                sq = blk * blk
                lane_part = sq if lane_part is None else lane_part + sq
                part = jnp.sum(sq.reshape(LANES // 8, 8, LANES), axis=0)
                acc[j] = part if acc[j] is None else acc[j] + part
            row_dst[row_me, s, c : c + 1, :] = jnp.sum(lane_part.T, axis=0, keepdims=True)
        for j in range(4):
            col_dst[col_me, s, j : j + 1, :] = jnp.sum(acc[j], axis=0, keepdims=True)

    def a_copies(gi):
        s0, n = GROUPS[gi]
        sl = pl.ds(s0, n)
        out = []
        for d in range(1, NA):
            out.append(
                pltpu.make_async_remote_copy(
                    src_ref=attbuf.at[a, sl], dst_ref=attbuf.at[a, sl],
                    send_sem=send_sem.at[0], recv_sem=a_recv.at[gi],
                    device_id=(lax.rem(a + d, NA), e), device_id_type=MESH,
                )
            )
            out.append(
                pltpu.make_async_remote_copy(
                    src_ref=embbuf.at[e, sl], dst_ref=embbuf.at[e, sl],
                    send_sem=send_sem.at[1], recv_sem=e_recv.at[gi],
                    device_id=(a, lax.rem(e + d, NE)), device_id_type=MESH,
                )
            )
        return out

    def wait_bytes(ref, sem):
        pltpu.make_async_copy(ref, ref, sem).wait()

    def a_wait(gi):
        s0, n = GROUPS[gi]
        wait_bytes(attbuf.at[pl.ds(0, NA - 1), pl.ds(s0, n)], a_recv.at[gi])
        wait_bytes(embbuf.at[pl.ds(0, NE - 1), pl.ds(s0, n)], e_recv.at[gi])

    def send_b(l):
        for d in range(1, NA * NE):
            da, de = divmod(d, NE)
            pltpu.make_async_remote_copy(
                src_ref=bbuf.at[l, me], dst_ref=bbuf.at[l, me],
                send_sem=send_sem.at[2], recv_sem=b_recv.at[l],
                device_id=(lax.rem(a + da, NA), lax.rem(e + de, NE)), device_id_type=MESH,
            ).start()

    lane = lax.broadcasted_iota(jnp.int32, (1, LANES), 1)

    def finish(s):
        l, m = divmod(s, 4)
        is_out = m == 3
        row_src, col_src = (embbuf, attbuf) if is_out else (attbuf, embbuf)
        beta = hp[0]
        one_beta = 1.0 - beta
        acc = [None] * 4
        r_sum = None
        for c in range(4):
            ls = pl.ds(c * LANES, LANES)
            tot = (row_src[0, s, c : c + 1, :] + row_src[1, s, c : c + 1, :]) + (
                row_src[2, s, c : c + 1, :] + row_src[3, s, c : c + 1, :]
            )
            old = ro_old[l : l + 1, ls] if is_out else rq_old[m, l : l + 1, ls]
            r_new = beta * old + one_beta * (tot * (1.0 / n_total) + EPS_SQUARE)
            if is_out:
                ro[l : l + 1, ls] = r_new
            else:
                rq[m, l : l + 1, ls] = r_new
            r_sum = r_new if r_sum is None else r_sum + r_new
            factor = col_of(lax.rsqrt(r_new))
            for j in range(4):
                t = g_at(s)[ls, pl.ds(j * LANES, LANES)] * factor
                part = jnp.sum((t * t).reshape(LANES // 8, 8, LANES), axis=0)
                acc[j] = part if acc[j] is None else acc[j] + part
        u = None
        for c in range(4):
            ls = pl.ds(c * LANES, LANES)
            tot = (col_src[0, s, c : c + 1, :] + col_src[1, s, c : c + 1, :]) + (
                col_src[2, s, c : c + 1, :] + col_src[3, s, c : c + 1, :]
            )
            old = co_old[l : l + 1, ls] if is_out else cq_old[m, l : l + 1, ls]
            c_new = beta * old + one_beta * (tot * (1.0 / n_total) + EPS_SQUARE)
            if is_out:
                co[l : l + 1, ls] = c_new
            else:
                cq[m, l : l + 1, ls] = c_new
            col_factor = lax.rsqrt(c_new)
            part = acc[c] * (col_factor * col_factor)
            u = part if u is None else u + part
        bbuf[l, me, m : m + 1, :] = jnp.sum(u, axis=0, keepdims=True)
        w_sum = wsq[s]
        bbuf[l, me, 4 + m : 5 + m, :] = jnp.where(
            lane < LANES // 2, w_sum + pltpu.roll(w_sum, LANES // 2, 1), r_sum + pltpu.roll(r_sum, LANES // 2, 1)
        )

    def pieces(s):
        l, m = divmod(s, 4)
        sl = [pl.ds(c * LANES, LANES) for c in range(4)]
        if m == 3:
            return [ro[l : l + 1, i] for i in sl], [co[l : l + 1, i] for i in sl]
        return [rq[m, l : l + 1, i] for i in sl], [cq[m, l : l + 1, i] for i in sl]

    steps = {}

    def gather_b(l):
        wait_bytes(bbuf.at[l, pl.ds(0, NA * NE - 1)], b_recv.at[l])
        tot = bbuf[l, 0]
        for d in range(1, NA * NE):
            tot = tot + bbuf[l, d]
        return tot

    def update(s):
        l, m = divmod(s, 4)
        if l not in steps:
            steps[l] = step_sizes(gather_b(l), n_total, hp[1], hp[2])
        rows, cols = pieces(s)
        update_one(wn.at[s], wn.at[s], g_at(s), rows, cols, steps[l][m : m + 1, :])

    wsq = {}

    def w_square(s):
        w_copy(s).wait()
        acc = None
        for c in range(4):
            for j in range(4):
                blk = w_at(s)[pl.ds(c * LANES, LANES), pl.ds(j * LANES, LANES)]
                part = jnp.sum((blk * blk).reshape(LANES // 8, 8, LANES), axis=0)
                acc = part if acc is None else acc + part
        wsq[s] = jnp.sum(acc, axis=0, keepdims=True)

    DN = (((0,), (0,)), ((), ()))
    for s in range(MATS):
        l, m = divmod(s, 4)
        xi = 2 * l + (m == 3)
        if s + 3 < MATS:
            nl, nm = divmod(s + 3, 4)
            if nm == 3 or nm == 0:
                x_copy(2 * nl + (nm == 3)).start()
            dy_copy(s + 3).start()
        w_copy(s).start()
        if s == 5:
            pl.semaphore_wait(barrier, NA * NE - 1)
        for gi, (s0, n) in enumerate(GROUPS):
            if s0 + n + 1 == s:
                for c in a_copies(gi):
                    c.start()
        if s == 8:
            for c in small:
                c.wait()
        if s in A_WAIT:
            a_wait(A_WAIT[s])
        if s in B_SEND:
            send_b(B_SEND[s])
        if s == 0:
            for k in range(KCH):
                rows = pl.ds(k * (TOK // KCH), TOK // KCH)
                for c in first_chunk(k):
                    c.wait()
                part = lax.dot_general(xbuf[0, rows], dybuf[0, rows], DN, preferred_element_type=F32)
                g_at(0)[...] = part if k == 0 else g_at(0)[...] + part
        else:
            if m == 0 or m == 3:
                x_copy(xi).wait()
            dy_copy(s).wait()
            g_at(s)[...] = lax.dot_general(xbuf[xi % NX], dybuf[s % NDY], DN, preferred_element_type=F32)
        if s >= 1:
            stats(s - 1)
        if s >= 2:
            w_square(s - 2)
        for t, at in FINISHES.items():
            if at == s:
                finish(t)
    for c in a_copies(4):
        c.start()
    send_b(1)
    stats(15)
    for c in a_copies(5):
        c.start()
    w_square(14)
    w_square(15)
    a_wait(2)
    for t in (8, 9, 10, 11):
        finish(t)
    send_b(2)
    a_wait(3)
    finish(12)
    finish(13)
    for t in (0, 1, 2, 3):
        update(t)
    a_wait(4)
    finish(14)
    a_wait(5)
    finish(15)
    send_b(3)
    for t in range(4, LAST):
        update(t)
    bs[...] = gather_b(3)
    wait_bytes(attbuf.at[pl.ds(0, NA - 1)], send_sem.at[0])
    wait_bytes(embbuf.at[pl.ds(0, NE - 1)], send_sem.at[1])
    wait_bytes(bbuf.at[:, pl.ds(0, NA * NE - 1)], send_sem.at[2])


def update_body(
    n_total, wn, g3, w3, rq, cq, ro, co, bs, hyper,
    w_qkv_new, w_out_new, rq_new, cq_new, ro_new, co_new,
    obuf, hp, osem, rsem, hsem,
):
    load_hp = pltpu.make_async_copy(hyper, hp, hsem)
    load_hp.start()

    def out_copy(s):
        l, m = divmod(s, 4)
        dst = w_out_new.at[l] if m == 3 else w_qkv_new.at[l, m]
        return pltpu.make_async_copy(obuf.at[s - LAST] if s >= LAST else wn.at[s], dst, osem.at[m // 3 if s < LAST else s - LAST + 2])

    for s in range(LAST):
        out_copy(s).start()
    small = [
        pltpu.make_async_copy(rq, rq_new, rsem.at[0]),
        pltpu.make_async_copy(cq, cq_new, rsem.at[1]),
        pltpu.make_async_copy(ro, ro_new, rsem.at[2]),
        pltpu.make_async_copy(co, co_new, rsem.at[3]),
    ]
    for c in small:
        c.start()
    load_hp.wait()
    l = LAYERS - 1
    step = step_sizes(bs[...], n_total, hp[1], hp[2])
    sl = [pl.ds(c * LANES, LANES) for c in range(4)]
    for m in range(4):
        if m == 3:
            rows, cols = [ro[l : l + 1, i] for i in sl], [co[l : l + 1, i] for i in sl]
        else:
            rows, cols = [rq[m, l : l + 1, i] for i in sl], [cq[m, l : l + 1, i] for i in sl]
        update_one(obuf.at[m], w3.at[m], g3.at[m], rows, cols, step[m : m + 1, :])
        out_copy(LAST + m).start()
    first = w_qkv_new.at[pl.ds(0, LAYERS - 1)]
    pltpu.make_async_copy(first, first, osem.at[0]).wait()
    first = w_out_new.at[pl.ds(0, LAYERS - 1)]
    pltpu.make_async_copy(first, first, osem.at[1]).wait()
    for s in range(LAST, MATS):
        out_copy(s).wait()
    for c in small:
        c.wait()


def solution(mesh):
    in_specs = (
        P(None, None, "emb", "att"),
        P(None, "att", "emb"),
        P(None, None, "emb"),
        P(None, None, None, "att"),
        P(None, None, "att"),
        P(None, None, "emb"),
        P(None, None, "emb"),
        P(None, None, "att"),
        P(None, "att"),
        P(None, "emb"),
        P(),
    )
    out_specs = (
        P(None, None, "emb", "att"),
        P(None, "att", "emb"),
        P(None, None, "emb"),
        P(None, None, "att"),
        P(None, "att"),
        P(None, "emb"),
    )
    n_total = B * NA
    hbm = pl.BlockSpec(memory_space=pltpu.HBM)
    vm = pl.BlockSpec(memory_space=pltpu.VMEM)
    dma = pltpu.SemaphoreType.DMA

    def local_run(w_qkv, w_out, x_in, dy_qkv, x_attn, dy_out, r_qkv, c_qkv, r_out, c_out, hyper_params):
        ng = len(GROUPS)
        swap = lambda v: jnp.transpose(v, (1, 0, 2))
        mid = pl.pallas_call(
            functools.partial(stats_body, n_total),
            out_shape=(
                pltpu.VMEM((LAST, B, B), F32),
                pltpu.VMEM((4, B, B), F32),
                pltpu.VMEM((4, B, B), F32),
                pltpu.VMEM((3, LAYERS, B), F32),
                pltpu.VMEM((3, LAYERS, B), F32),
                pltpu.VMEM((LAYERS, B), F32),
                pltpu.VMEM((LAYERS, B), F32),
                pltpu.VMEM((8, LANES), F32),
            ),
            in_specs=[hbm] * 11,
            out_specs=(vm,) * 8,
            scratch_shapes=[
                pltpu.VMEM((NX, TOK, B), BF16),
                pltpu.VMEM((NDY, TOK, B), BF16),
                pltpu.VMEM((NA, MATS, 4, LANES), F32),
                pltpu.VMEM((NE, MATS, 4, LANES), F32),
                pltpu.VMEM((LAYERS, NA * NE, 8, LANES), F32),
                pltpu.VMEM((3, LAYERS, B), F32),
                pltpu.VMEM((3, LAYERS, B), F32),
                pltpu.VMEM((LAYERS, B), F32),
                pltpu.VMEM((LAYERS, B), F32),
                pltpu.SMEM((3,), F32),
                pltpu.VMEM((NG, B, B), F32),
                dma((NX,)),
                dma((NDY,)),
                dma((NW,)),
                dma((5,)),
                dma((2 * KCH,)),
                dma((3,)),
                dma((ng,)),
                dma((ng,)),
                dma((LAYERS,)),
            ],
            compiler_params=pltpu.CompilerParams(
                collective_id=0, has_side_effects=True, vmem_limit_bytes=36 * 2**20
            ),
            name="stats",
        )(w_qkv, w_out, x_in, dy_qkv, x_attn, dy_out, swap(r_qkv), swap(c_qkv), r_out, c_out, hyper_params)
        new = pl.pallas_call(
            functools.partial(update_body, n_total),
            out_shape=(
                jax.ShapeDtypeStruct(w_qkv.shape, F32),
                jax.ShapeDtypeStruct(w_out.shape, F32),
                jax.ShapeDtypeStruct((3, LAYERS, B), F32),
                jax.ShapeDtypeStruct((3, LAYERS, B), F32),
                jax.ShapeDtypeStruct(r_out.shape, F32),
                jax.ShapeDtypeStruct(c_out.shape, F32),
            ),
            in_specs=[vm] * 8 + [hbm],
            out_specs=(hbm,) * 6,
            scratch_shapes=[
                pltpu.VMEM((4, B, B), F32),
                pltpu.SMEM((3,), F32),
                dma((6,)),
                dma((4,)),
                dma,
            ],
            compiler_params=pltpu.CompilerParams(vmem_limit_bytes=6 * 2**20),
            name="update",
        )(*mid, hyper_params)
        return new[0], new[1], swap(new[2]), swap(new[3]), new[4], new[5]

    return jax.shard_map(local_run, mesh=mesh, in_specs=in_specs, out_specs=out_specs, check_vma=False)
```

```python
import functools

import jax
import jax.numpy as jnp
from jax import lax
from jax.experimental import pallas as pl
from jax.experimental.pallas import tpu as pltpu
from jax.sharding import PartitionSpec as P

EPS_SQUARE = 1e-30
EPS_SCALE = 1e-3
MESH = pl.DeviceIdType.MESH
F32 = jnp.float32
BF16 = jnp.bfloat16
NA = 4
NE = 4
LAYERS = 4
MATS = 16
TOK = 2048
B = 512
LANES = 128
NDY = 8
NX = 5
NW = 16
KCH = 4
LAST = 12
NG = 12
GROUPS = ((0, 4), (4, 4), (8, 4), (12, 3), (15, 1))


SLOTS = ((0,), (1,), (2,), (3,), (4, 5), (6, 7), (8, 9, 10), (11, 12, 13), (14, 15))
AHEAD = 7
W_ASK = {6: 1, 7: 4, 8: 16}
W_SQUARE = {8: 4}
FIRST_SEND = 5
A_SEND = {5: 0, 7: 1, 8: 2}
A_WAIT = {7: 0, 8: 1}
FINISHES = {7: (0, 1, 2, 3), 8: (4, 5, 6, 7)}
TILES = ((0, 8), (8, 4), (12, 4))
STRIDE = 8


def place(s):
    return (s - LAST, 3) if s >= LAST else divmod(s, 3)


def x_index(s):
    return s - 8 if s >= LAST else s // 3


def new_x(s):
    return s >= LAST or s % 3 == 0


def col_of(row_piece):
    return jnp.broadcast_to(row_piece, (LANES, LANES)).T


def step_sizes(tot, n_total, rho, clip):
    n_elems = float(n_total) * float(n_total)
    w_sum = pltpu.roll(tot, LANES - STRIDE, 1)
    r_mean = pltpu.roll(tot, LANES - 2 * STRIDE, 1) * (0.25 / n_total)
    rms_u = jnp.sqrt(tot * r_mean / n_elems)
    rms_w = jnp.sqrt(w_sum / n_elems)
    return rho * jnp.maximum(EPS_SCALE, rms_w) * jnp.sqrt(r_mean) / jnp.maximum(1.0, rms_u / clip)


def update_one(dst, w_ref, g_ref, row_pieces, col_pieces, st):
    cols = [lax.rsqrt(c_new) * st for c_new in col_pieces]
    for c in range(4):
        ls = pl.ds(c * LANES, LANES)
        factor = col_of(lax.rsqrt(row_pieces[c]))
        for j in range(4):
            js = pl.ds(j * LANES, LANES)
            dst[ls, js] = w_ref[ls, js] - (g_ref[ls, js] * factor) * cols[j]


def stats_body(
    n_total,
    w_qkv, w_out, x_in, dy_qkv, x_attn, dy_out, r_qkv, c_qkv, r_out, c_out, hyper,
    wn, g3, w3, rq, cq, ro, co, bs,
    xbuf, dybuf, attbuf, embbuf, bbuf, rq_old, cq_old, ro_old, co_old, hp, gring,
    xsem, dysem, wsem, insem, ch_sem, send_sem, a_recv, e_recv, b_recv,
):
    a = lax.axis_index("att")
    e = lax.axis_index("emb")
    me = a * NE + e

    barrier = pltpu.get_barrier_semaphore()
    for da in range(NA):
        for de in range(NE):
            if da or de:
                pl.semaphore_signal(
                    barrier, inc=1, device_id=(lax.rem(a + da, NA), lax.rem(e + de, NE)), device_id_type=MESH
                )

    def g_at(s):
        return g3.at[s - LAST] if s >= LAST else gring.at[s % NG]

    def w_at(s):
        return w3.at[s - LAST] if s >= LAST else wn.at[s]

    def x_copy(xi):
        src = x_attn.at[xi - LAYERS] if xi >= LAYERS else x_in.at[xi]
        return pltpu.make_async_copy(src, xbuf.at[xi % NX], xsem.at[xi % NX])

    def dy_copy(s):
        l, m = place(s)
        src = dy_out.at[l] if m == 3 else dy_qkv.at[l, m]
        return pltpu.make_async_copy(src, dybuf.at[s % NDY], dysem.at[s % NDY])

    def w_copy(s):
        l, m = place(s)
        src = w_out.at[l] if m == 3 else w_qkv.at[l, m]
        return pltpu.make_async_copy(src, w_at(s), wsem.at[s % NW])

    def first_chunk(k):
        rows = pl.ds(k * (TOK // KCH), TOK // KCH)
        return (
            pltpu.make_async_copy(x_in.at[0, rows], xbuf.at[0, rows], ch_sem.at[2 * k]),
            pltpu.make_async_copy(dy_qkv.at[0, 0, rows], dybuf.at[0, rows], ch_sem.at[2 * k + 1]),
        )

    small = [
        pltpu.make_async_copy(r_qkv, rq_old, insem.at[0]),
        pltpu.make_async_copy(c_qkv, cq_old, insem.at[1]),
        pltpu.make_async_copy(r_out, ro_old, insem.at[2]),
        pltpu.make_async_copy(c_out, co_old, insem.at[3]),
        pltpu.make_async_copy(hyper, hp, insem.at[4]),
    ]

    for k in range(KCH):
        for c in first_chunk(k):
            c.start()
    dy_copy(1).start()
    dy_copy(2).start()
    for c in small:
        c.start()

    def stats(s):
        is_out = s >= LAST
        row_dst, row_me = (embbuf, e) if is_out else (attbuf, a)
        col_dst, col_me = (attbuf, a) if is_out else (embbuf, e)
        acc = [None] * 4
        for c in range(4):
            rows = pl.ds(c * LANES, LANES)
            lane_part = None
            for j in range(4):
                blk = g_at(s)[rows, pl.ds(j * LANES, LANES)]
                sq = blk * blk
                lane_part = sq if lane_part is None else lane_part + sq
                part = jnp.sum(sq.reshape(LANES // 8, 8, LANES), axis=0)
                acc[j] = part if acc[j] is None else acc[j] + part
            row_dst[row_me, s, c : c + 1, :] = jnp.sum(lane_part.T, axis=0, keepdims=True)
        for j in range(4):
            col_dst[col_me, s, j : j + 1, :] = jnp.sum(acc[j], axis=0, keepdims=True)

    def a_copies(gi):
        s0, n = GROUPS[gi]
        sl = pl.ds(s0, n)
        out = []
        for d in range(1, NA):
            out.append(
                pltpu.make_async_remote_copy(
                    src_ref=attbuf.at[a, sl], dst_ref=attbuf.at[a, sl],
                    send_sem=send_sem.at[0], recv_sem=a_recv.at[gi],
                    device_id=(lax.rem(a + d, NA), e), device_id_type=MESH,
                )
            )
            out.append(
                pltpu.make_async_remote_copy(
                    src_ref=embbuf.at[e, sl], dst_ref=embbuf.at[e, sl],
                    send_sem=send_sem.at[1], recv_sem=e_recv.at[gi],
                    device_id=(a, lax.rem(e + d, NE)), device_id_type=MESH,
                )
            )
        return out

    def wait_bytes(ref, sem):
        pltpu.make_async_copy(ref, ref, sem).wait()

    def a_wait(gi):
        s0, n = GROUPS[gi]
        wait_bytes(attbuf.at[pl.ds(0, NA - 1), pl.ds(s0, n)], a_recv.at[gi])
        wait_bytes(embbuf.at[pl.ds(0, NE - 1), pl.ds(s0, n)], e_recv.at[gi])

    def send_b(l):
        for d in range(1, NA * NE):
            da, de = divmod(d, NE)
            pltpu.make_async_remote_copy(
                src_ref=bbuf.at[l, me], dst_ref=bbuf.at[l, me],
                send_sem=send_sem.at[2], recv_sem=b_recv.at[l],
                device_id=(lax.rem(a + da, NA), lax.rem(e + de, NE)), device_id_type=MESH,
            ).start()

    lane = lax.broadcasted_iota(jnp.int32, (1, LANES), 1)

    def finish(s):
        l, m = place(s)
        is_out = m == 3
        row_src, col_src = (embbuf, attbuf) if is_out else (attbuf, embbuf)
        beta = hp[0]
        one_beta = 1.0 - beta
        acc = [None] * 4
        r_sum = None
        for c in range(4):
            ls = pl.ds(c * LANES, LANES)
            tot = (row_src[0, s, c : c + 1, :] + row_src[1, s, c : c + 1, :]) + (
                row_src[2, s, c : c + 1, :] + row_src[3, s, c : c + 1, :]
            )
            old = ro_old[l : l + 1, ls] if is_out else rq_old[m, l : l + 1, ls]
            r_new = beta * old + one_beta * (tot * (1.0 / n_total) + EPS_SQUARE)
            if is_out:
                ro[l : l + 1, ls] = r_new
            else:
                rq[m, l : l + 1, ls] = r_new
            r_sum = r_new if r_sum is None else r_sum + r_new
            factor = col_of(lax.rsqrt(r_new))
            for j in range(4):
                t = g_at(s)[ls, pl.ds(j * LANES, LANES)] * factor
                part = jnp.sum((t * t).reshape(LANES // 8, 8, LANES), axis=0)
                acc[j] = part if acc[j] is None else acc[j] + part
        u = None
        for c in range(4):
            ls = pl.ds(c * LANES, LANES)
            tot = (col_src[0, s, c : c + 1, :] + col_src[1, s, c : c + 1, :]) + (
                col_src[2, s, c : c + 1, :] + col_src[3, s, c : c + 1, :]
            )
            old = co_old[l : l + 1, ls] if is_out else cq_old[m, l : l + 1, ls]
            c_new = beta * old + one_beta * (tot * (1.0 / n_total) + EPS_SQUARE)
            if is_out:
                co[l : l + 1, ls] = c_new
            else:
                cq[m, l : l + 1, ls] = c_new
            col_factor = lax.rsqrt(c_new)
            part = acc[c] * (col_factor * col_factor)
            u = part if u is None else u + part
        u_sums[s] = jnp.sum(jnp.sum(u, axis=0, keepdims=True), axis=1, keepdims=True)
        r_sums[s] = jnp.sum(r_sum, axis=1, keepdims=True)

    u_sums, r_sums = {}, {}

    def pack(l):
        row = jnp.zeros((1, LANES), F32)
        s0, n = TILES[l]
        for k, sums in enumerate((u_sums, wsq, r_sums)):
            for i in range(n):
                row = jnp.where(lane == STRIDE * k + i, sums[s0 + i], row)
        bbuf[l, me] = row
        send_b(l)

    def pieces(s):
        l, m = place(s)
        sl = [pl.ds(c * LANES, LANES) for c in range(4)]
        if m == 3:
            return [ro[l : l + 1, i] for i in sl], [co[l : l + 1, i] for i in sl]
        return [rq[m, l : l + 1, i] for i in sl], [cq[m, l : l + 1, i] for i in sl]

    steps = {}

    def gather_b(l):
        wait_bytes(bbuf.at[l, pl.ds(0, NA * NE - 1)], b_recv.at[l])
        tot = bbuf[l, 0]
        for d in range(1, NA * NE):
            tot = tot + bbuf[l, d]
        return tot

    def update(s):
        l = 0 if s < TILES[1][0] else 1
        m = s - TILES[l][0]
        if l not in steps:
            steps[l] = step_sizes(gather_b(l), n_total, hp[1], hp[2])
        rows, cols = pieces(s)
        update_one(wn.at[s], wn.at[s], g_at(s), rows, cols, steps[l][:, m : m + 1])

    wsq = {}

    def w_square(s):
        acc = None
        for c in range(4):
            for j in range(4):
                blk = w_at(s)[pl.ds(c * LANES, LANES), pl.ds(j * LANES, LANES)]
                part = jnp.sum((blk * blk).reshape(LANES // 8, 8, LANES), axis=0)
                acc = part if acc is None else acc + part
        wsq[s] = jnp.sum(jnp.sum(acc, axis=0, keepdims=True), axis=1, keepdims=True)

    DN = (((0,), (0,)), ((), ()))
    asked = 3
    w_asked = 0
    squared = 0
    for slot, dots in enumerate(SLOTS):
        while asked < min(dots[0] + AHEAD, MATS):
            if new_x(asked):
                x_copy(x_index(asked)).start()
            dy_copy(asked).start()
            asked += 1
        while w_asked < W_ASK.get(slot, 0):
            w_copy(w_asked).start()
            w_asked += 1
        if slot == FIRST_SEND:
            pl.semaphore_wait(barrier, NA * NE - 1)
        if slot in A_SEND:
            for c in a_copies(A_SEND[slot]):
                c.start()
        w_ready = W_SQUARE.get(slot, 0)
        if slot == 7:
            for c in small:
                c.wait()
        if slot in A_WAIT:
            a_wait(A_WAIT[slot])
        for t in range(squared, w_ready):
            w_copy(t).wait()
        if slot:
            for s in dots:
                if new_x(s):
                    x_copy(x_index(s)).wait()
                dy_copy(s).wait()
        for s in dots:
            xi = x_index(s)
            if s == 0:
                for k in range(KCH):
                    rows = pl.ds(k * (TOK // KCH), TOK // KCH)
                    for c in first_chunk(k):
                        c.wait()
                    part = lax.dot_general(xbuf[0, rows], dybuf[0, rows], DN, preferred_element_type=F32)
                    g_at(0)[...] = part if k == 0 else g_at(0)[...] + part
            else:
                g_at(s)[...] = lax.dot_general(xbuf[xi % NX], dybuf[s % NDY], DN, preferred_element_type=F32)
                stats(s - 1)
        for t in range(squared, w_ready):
            w_square(t)
        squared = max(squared, w_ready)
        for t in FINISHES.get(slot, ()):
            finish(t)

    for c in a_copies(3):
        c.start()
    stats(15)
    for c in a_copies(4):
        c.start()

    def square_more(s0):
        for t in range(s0, s0 + 4):
            w_copy(t).wait()
        for t in range(s0, s0 + 4):
            w_square(t)

    square_more(4)
    pack(0)
    a_wait(2)
    square_more(8)
    for t in (8, 9, 10, 11):
        finish(t)
    pack(1)
    square_more(12)
    a_wait(3)
    a_wait(4)
    for t in (12, 13, 14, 15):
        finish(t)
    pack(2)
    for t in range(LAST):
        update(t)
    bs[...] = gather_b(2)
    wait_bytes(attbuf.at[pl.ds(0, NA - 1)], send_sem.at[0])
    wait_bytes(embbuf.at[pl.ds(0, NE - 1)], send_sem.at[1])
    wait_bytes(bbuf.at[:, pl.ds(0, NA * NE - 1)], send_sem.at[2])


def update_body(
    n_total, wn, g3, w3, rq, cq, ro, co, bs, hyper,
    w_qkv_new, w_out_new, rq_new, cq_new, ro_new, co_new,
    obuf, hp, osem, rsem, hsem,
):
    load_hp = pltpu.make_async_copy(hyper, hp, hsem)
    load_hp.start()

    first = []
    for s in range(LAST):
        l, m = place(s)
        first.append(pltpu.make_async_copy(wn.at[s], w_qkv_new.at[l, m], osem.at[0]))
        first[-1].start()
    small = [
        pltpu.make_async_copy(rq, rq_new, rsem.at[0]),
        pltpu.make_async_copy(cq, cq_new, rsem.at[1]),
        pltpu.make_async_copy(ro, ro_new, rsem.at[2]),
        pltpu.make_async_copy(co, co_new, rsem.at[3]),
    ]
    for c in small:
        c.start()
    load_hp.wait()
    step = step_sizes(bs[...], n_total, hp[1], hp[2])
    sl = [pl.ds(c * LANES, LANES) for c in range(4)]
    last = []
    for l in range(LAYERS):
        rows, cols = [ro[l : l + 1, i] for i in sl], [co[l : l + 1, i] for i in sl]
        update_one(obuf.at[l], w3.at[l], g3.at[l], rows, cols, step[:, l : l + 1])
        last.append(pltpu.make_async_copy(obuf.at[l], w_out_new.at[l], osem.at[1 + l]))
        last[-1].start()
    pltpu.make_async_copy(w_qkv_new, w_qkv_new, osem.at[0]).wait()
    for c in last + small:
        c.wait()


def solution(mesh):
    in_specs = (
        P(None, None, "emb", "att"),
        P(None, "att", "emb"),
        P(None, None, "emb"),
        P(None, None, None, "att"),
        P(None, None, "att"),
        P(None, None, "emb"),
        P(None, None, "emb"),
        P(None, None, "att"),
        P(None, "att"),
        P(None, "emb"),
        P(),
    )
    out_specs = (
        P(None, None, "emb", "att"),
        P(None, "att", "emb"),
        P(None, None, "emb"),
        P(None, None, "att"),
        P(None, "att"),
        P(None, "emb"),
    )
    n_total = B * NA
    hbm = pl.BlockSpec(memory_space=pltpu.HBM)
    vm = pl.BlockSpec(memory_space=pltpu.VMEM)
    dma = pltpu.SemaphoreType.DMA

    def local_run(w_qkv, w_out, x_in, dy_qkv, x_attn, dy_out, r_qkv, c_qkv, r_out, c_out, hyper_params):
        ng = len(GROUPS)
        swap = lambda v: jnp.transpose(v, (1, 0, 2))
        mid = pl.pallas_call(
            functools.partial(stats_body, n_total),
            out_shape=(
                pltpu.VMEM((LAST, B, B), F32),
                pltpu.VMEM((4, B, B), F32),
                pltpu.VMEM((4, B, B), F32),
                pltpu.VMEM((3, LAYERS, B), F32),
                pltpu.VMEM((3, LAYERS, B), F32),
                pltpu.VMEM((LAYERS, B), F32),
                pltpu.VMEM((LAYERS, B), F32),
                pltpu.VMEM((1, LANES), F32),
            ),
            in_specs=[hbm] * 11,
            out_specs=(vm,) * 8,
            scratch_shapes=[
                pltpu.VMEM((NX, TOK, B), BF16),
                pltpu.VMEM((NDY, TOK, B), BF16),
                pltpu.VMEM((NA, MATS, 4, LANES), F32),
                pltpu.VMEM((NE, MATS, 4, LANES), F32),
                pltpu.VMEM((len(TILES), NA * NE, 1, LANES), F32),
                pltpu.VMEM((3, LAYERS, B), F32),
                pltpu.VMEM((3, LAYERS, B), F32),
                pltpu.VMEM((LAYERS, B), F32),
                pltpu.VMEM((LAYERS, B), F32),
                pltpu.SMEM((3,), F32),
                pltpu.VMEM((NG, B, B), F32),
                dma((NX,)),
                dma((NDY,)),
                dma((NW,)),
                dma((5,)),
                dma((2 * KCH,)),
                dma((3,)),
                dma((ng,)),
                dma((ng,)),
                dma((len(TILES),)),
            ],
            compiler_params=pltpu.CompilerParams(
                collective_id=0, has_side_effects=True, vmem_limit_bytes=42 * 2**20
            ),
            name="stats",
        )(w_qkv, w_out, x_in, dy_qkv, x_attn, dy_out, swap(r_qkv), swap(c_qkv), r_out, c_out, hyper_params)
        new = pl.pallas_call(
            functools.partial(update_body, n_total),
            out_shape=(
                jax.ShapeDtypeStruct(w_qkv.shape, F32),
                jax.ShapeDtypeStruct(w_out.shape, F32),
                jax.ShapeDtypeStruct((3, LAYERS, B), F32),
                jax.ShapeDtypeStruct((3, LAYERS, B), F32),
                jax.ShapeDtypeStruct(r_out.shape, F32),
                jax.ShapeDtypeStruct(c_out.shape, F32),
            ),
            in_specs=[vm] * 8 + [hbm],
            out_specs=(hbm,) * 6,
            scratch_shapes=[
                pltpu.VMEM((4, B, B), F32),
                pltpu.SMEM((3,), F32),
                dma((1 + LAYERS,)),
                dma((4,)),
                dma,
            ],
            compiler_params=pltpu.CompilerParams(vmem_limit_bytes=6 * 2**20),
            name="update",
        )(*mid, hyper_params)
        return new[0], new[1], swap(new[2]), swap(new[3]), new[4], new[5]

    return jax.shard_map(local_run, mesh=mesh, in_specs=in_specs, out_specs=out_specs, check_vma=False)
```

```python
import functools

import jax
import jax.numpy as jnp
from jax import lax
from jax.experimental import pallas as pl
from jax.experimental.pallas import tpu as pltpu
from jax.sharding import PartitionSpec as P

EPS_SQUARE = 1e-30
EPS_SCALE = 1e-3
MESH = pl.DeviceIdType.MESH
F32 = jnp.float32
BF16 = jnp.bfloat16
NA = 4
NE = 4
LAYERS = 4
MATS = 16
TOK = 2048
B = 512
LANES = 128
NDY = 8
NX = 5
NW = 4
KCH = 4
LAST = 12
NG = 12
GROUPS = ((0, 4), (4, 4), (8, 4), (12, 3), (15, 1))


SLOTS = ((0,), (1,), (2,), (3,), (4, 5), (6, 7), (8, 9, 10), (11, 12, 13), (14, 15))
AHEAD = 7
W_ASK = {6: 1, 7: 4, 8: 16}
W_SQUARE = {8: 4}
FIRST_SEND = 5
A_SEND = {5: 0, 7: 1, 8: 2}
A_WAIT = {7: 0, 8: 1}
FINISHES = {7: (0, 1, 2, 3), 8: (4, 5, 6, 7)}
TILES = ((0, 8), (8, 4), (12, 4))
STRIDE = 8
FAR_FIRST = tuple((da, de) for da in (1, 3, 2, 0) for de in (1, 3, 2, 0) if da or de)


def place(s):
    return (s - LAST, 3) if s >= LAST else divmod(s, 3)


def x_index(s):
    return s - 8 if s >= LAST else s // 3


def new_x(s):
    return s >= LAST or s % 3 == 0


def col_of(row_piece):
    return jnp.broadcast_to(row_piece, (LANES, LANES)).T


def step_sizes(tot, n_total, rho, clip):
    n_elems = float(n_total) * float(n_total)
    w_sum = pltpu.roll(tot, LANES - STRIDE, 1)
    r_mean = pltpu.roll(tot, LANES - 2 * STRIDE, 1) * (0.25 / n_total)
    rms_u = jnp.sqrt(tot * r_mean / n_elems)
    rms_w = jnp.sqrt(w_sum / n_elems)
    return rho * jnp.maximum(EPS_SCALE, rms_w) * jnp.sqrt(r_mean) / jnp.maximum(1.0, rms_u / clip)


def update_one(dst, w_ref, g_ref, row_pieces, col_pieces, st):
    cols = [lax.rsqrt(c_new) * st for c_new in col_pieces]
    for c in range(4):
        ls = pl.ds(c * LANES, LANES)
        factor = col_of(lax.rsqrt(row_pieces[c]))
        for j in range(4):
            js = pl.ds(j * LANES, LANES)
            dst[ls, js] = w_ref[ls, js] - (g_ref[ls, js] * factor) * cols[j]


def stats_body(
    n_total,
    w_qkv, w_out, x_in, dy_qkv, x_attn, dy_out, r_qkv, c_qkv, r_out, c_out, hyper,
    wn, g3, w3, rq, cq, ro, co, bs,
    xbuf, dybuf, attbuf, embbuf, bbuf, rq_old, cq_old, ro_old, co_old, hp, gring,
    xsem, dysem, wsem, insem, ch_sem, send_sem, a_recv, e_recv, b_recv,
):
    a = lax.axis_index("att")
    e = lax.axis_index("emb")
    me = a * NE + e

    barrier = pltpu.get_barrier_semaphore()
    for da in range(NA):
        for de in range(NE):
            if da or de:
                pl.semaphore_signal(
                    barrier, inc=1, device_id=(lax.rem(a + da, NA), lax.rem(e + de, NE)), device_id_type=MESH
                )

    def g_at(s):
        return g3.at[s - LAST] if s >= LAST else gring.at[s % NG]

    def w_at(s):
        return w3.at[s - LAST] if s >= LAST else wn.at[s]

    def x_copy(xi):
        src = x_attn.at[xi - LAYERS] if xi >= LAYERS else x_in.at[xi]
        return pltpu.make_async_copy(src, xbuf.at[xi % NX], xsem.at[xi % NX])

    def dy_copy(s):
        l, m = place(s)
        src = dy_out.at[l] if m == 3 else dy_qkv.at[l, m]
        return pltpu.make_async_copy(src, dybuf.at[s % NDY], dysem.at[s % NDY])

    def w_copy(s):
        l, m = place(s)
        src = w_out.at[l] if m == 3 else w_qkv.at[l, m]
        return pltpu.make_async_copy(src, w_at(s), wsem.at[s // 4])

    def first_chunk(k):
        rows = pl.ds(k * (TOK // KCH), TOK // KCH)
        return (
            pltpu.make_async_copy(x_in.at[0, rows], xbuf.at[0, rows], ch_sem.at[k]),
            pltpu.make_async_copy(dy_qkv.at[0, 0, rows], dybuf.at[0, rows], ch_sem.at[k]),
        )

    small = [
        pltpu.make_async_copy(r_qkv, rq_old, insem.at[0]),
        pltpu.make_async_copy(c_qkv, cq_old, insem.at[1]),
        pltpu.make_async_copy(r_out, ro_old, insem.at[2]),
        pltpu.make_async_copy(c_out, co_old, insem.at[3]),
        pltpu.make_async_copy(hyper, hp, insem.at[4]),
    ]

    for k in range(KCH):
        for c in first_chunk(k):
            c.start()
    dy_copy(1).start()
    dy_copy(2).start()
    for c in small:
        c.start()

    def stats(s):
        is_out = s >= LAST
        row_dst, row_me = (embbuf, e) if is_out else (attbuf, a)
        col_dst, col_me = (attbuf, a) if is_out else (embbuf, e)
        acc = [None] * 4
        for c in range(4):
            rows = pl.ds(c * LANES, LANES)
            lane_part = None
            for j in range(4):
                blk = g_at(s)[rows, pl.ds(j * LANES, LANES)]
                sq = blk * blk
                lane_part = sq if lane_part is None else lane_part + sq
                part = jnp.sum(sq.reshape(LANES // 8, 8, LANES), axis=0)
                acc[j] = part if acc[j] is None else acc[j] + part
            row_dst[row_me, s, c : c + 1, :] = jnp.sum(lane_part.T, axis=0, keepdims=True)
        for j in range(4):
            col_dst[col_me, s, j : j + 1, :] = jnp.sum(acc[j], axis=0, keepdims=True)

    def a_copies(gi):
        s0, n = GROUPS[gi]
        sl = pl.ds(s0, n)
        out = []
        for d in (1, 3, 2):
            out.append(
                pltpu.make_async_remote_copy(
                    src_ref=attbuf.at[a, sl], dst_ref=attbuf.at[a, sl],
                    send_sem=send_sem.at[0], recv_sem=a_recv.at[gi],
                    device_id=(lax.rem(a + d, NA), e), device_id_type=MESH,
                )
            )
            out.append(
                pltpu.make_async_remote_copy(
                    src_ref=embbuf.at[e, sl], dst_ref=embbuf.at[e, sl],
                    send_sem=send_sem.at[1], recv_sem=e_recv.at[gi],
                    device_id=(a, lax.rem(e + d, NE)), device_id_type=MESH,
                )
            )
        return out

    def wait_bytes(ref, sem):
        pltpu.make_async_copy(ref, ref, sem).wait()

    def a_wait(gi):
        s0, n = GROUPS[gi]
        wait_bytes(attbuf.at[pl.ds(0, NA - 1), pl.ds(s0, n)], a_recv.at[gi])
        wait_bytes(embbuf.at[pl.ds(0, NE - 1), pl.ds(s0, n)], e_recv.at[gi])

    def send_b(l):
        for da, de in FAR_FIRST:
            pltpu.make_async_remote_copy(
                src_ref=bbuf.at[l, me], dst_ref=bbuf.at[l, me],
                send_sem=send_sem.at[2], recv_sem=b_recv.at[l],
                device_id=(lax.rem(a + da, NA), lax.rem(e + de, NE)), device_id_type=MESH,
            ).start()

    lane = lax.broadcasted_iota(jnp.int32, (1, LANES), 1)

    def finish(s):
        l, m = place(s)
        is_out = m == 3
        row_src, col_src = (embbuf, attbuf) if is_out else (attbuf, embbuf)
        beta = hp[0]
        one_beta = 1.0 - beta
        acc = [None] * 4
        r_sum = None
        for c in range(4):
            ls = pl.ds(c * LANES, LANES)
            tot = (row_src[0, s, c : c + 1, :] + row_src[1, s, c : c + 1, :]) + (
                row_src[2, s, c : c + 1, :] + row_src[3, s, c : c + 1, :]
            )
            old = ro_old[l : l + 1, ls] if is_out else rq_old[m, l : l + 1, ls]
            r_new = beta * old + one_beta * (tot * (1.0 / n_total) + EPS_SQUARE)
            if is_out:
                ro[l : l + 1, ls] = r_new
            else:
                rq[m, l : l + 1, ls] = r_new
            r_sum = r_new if r_sum is None else r_sum + r_new
            factor = col_of(lax.rsqrt(r_new))
            for j in range(4):
                t = g_at(s)[ls, pl.ds(j * LANES, LANES)] * factor
                part = jnp.sum((t * t).reshape(LANES // 8, 8, LANES), axis=0)
                acc[j] = part if acc[j] is None else acc[j] + part
        u = None
        for c in range(4):
            ls = pl.ds(c * LANES, LANES)
            tot = (col_src[0, s, c : c + 1, :] + col_src[1, s, c : c + 1, :]) + (
                col_src[2, s, c : c + 1, :] + col_src[3, s, c : c + 1, :]
            )
            old = co_old[l : l + 1, ls] if is_out else cq_old[m, l : l + 1, ls]
            c_new = beta * old + one_beta * (tot * (1.0 / n_total) + EPS_SQUARE)
            if is_out:
                co[l : l + 1, ls] = c_new
            else:
                cq[m, l : l + 1, ls] = c_new
            col_factor = lax.rsqrt(c_new)
            part = acc[c] * (col_factor * col_factor)
            u = part if u is None else u + part
        u_sums[s] = jnp.sum(jnp.sum(u, axis=0, keepdims=True), axis=1, keepdims=True)
        r_sums[s] = jnp.sum(r_sum, axis=1, keepdims=True)

    u_sums, r_sums = {}, {}

    def pack(l):
        row = jnp.zeros((1, LANES), F32)
        s0, n = TILES[l]
        for k, sums in enumerate((u_sums, wsq, r_sums)):
            for i in range(n):
                row = jnp.where(lane == STRIDE * k + i, sums[s0 + i], row)
        bbuf[l, me] = row
        send_b(l)

    def pieces(s):
        l, m = place(s)
        sl = [pl.ds(c * LANES, LANES) for c in range(4)]
        if m == 3:
            return [ro[l : l + 1, i] for i in sl], [co[l : l + 1, i] for i in sl]
        return [rq[m, l : l + 1, i] for i in sl], [cq[m, l : l + 1, i] for i in sl]

    steps = {}

    def gather_b(l):
        wait_bytes(bbuf.at[l, pl.ds(0, NA * NE - 1)], b_recv.at[l])
        tot = bbuf[l, 0]
        for d in range(1, NA * NE):
            tot = tot + bbuf[l, d]
        return tot

    def update(s):
        l = 0 if s < TILES[1][0] else 1
        m = s - TILES[l][0]
        if l not in steps:
            steps[l] = step_sizes(gather_b(l), n_total, hp[1], hp[2])
        rows, cols = pieces(s)
        update_one(wn.at[s], wn.at[s], g_at(s), rows, cols, steps[l][:, m : m + 1])

    wsq = {}

    def w_square(s):
        acc = None
        for c in range(4):
            for j in range(4):
                blk = w_at(s)[pl.ds(c * LANES, LANES), pl.ds(j * LANES, LANES)]
                part = jnp.sum((blk * blk).reshape(LANES // 8, 8, LANES), axis=0)
                acc = part if acc is None else acc + part
        wsq[s] = jnp.sum(jnp.sum(acc, axis=0, keepdims=True), axis=1, keepdims=True)

    DN = (((0,), (0,)), ((), ()))
    asked = 3
    w_asked = 0
    squared = 0
    for slot, dots in enumerate(SLOTS):
        while asked < min(dots[0] + AHEAD, MATS):
            if new_x(asked):
                x_copy(x_index(asked)).start()
            dy_copy(asked).start()
            asked += 1
        while w_asked < W_ASK.get(slot, 0):
            w_copy(w_asked).start()
            w_asked += 1
        if slot == FIRST_SEND:
            pl.semaphore_wait(barrier, NA * NE - 1)
        if slot in A_SEND:
            for c in a_copies(A_SEND[slot]):
                c.start()
        w_ready = W_SQUARE.get(slot, 0)
        if slot == 7:
            for c in small:
                c.wait()
        if slot in A_WAIT:
            a_wait(A_WAIT[slot])
        if w_ready > squared:
            wait_bytes(gring.at[pl.ds(0, 4)], wsem.at[0])
        if slot:
            for s in dots:
                if new_x(s):
                    x_copy(x_index(s)).wait()
                dy_copy(s).wait()
        for s in dots:
            xi = x_index(s)
            if s == 0:
                for k in range(KCH):
                    rows = pl.ds(k * (TOK // KCH), TOK // KCH)
                    wait_bytes(xbuf.at[0, pl.ds(0, 2 * TOK // KCH)], ch_sem.at[k])
                    part = lax.dot_general(xbuf[0, rows], dybuf[0, rows], DN, preferred_element_type=F32)
                    g_at(0)[...] = part if k == 0 else g_at(0)[...] + part
            else:
                g_at(s)[...] = lax.dot_general(xbuf[xi % NX], dybuf[s % NDY], DN, preferred_element_type=F32)
                stats(s - 1)
        for t in range(squared, w_ready):
            w_square(t)
        squared = max(squared, w_ready)
        for t in FINISHES.get(slot, ()):
            finish(t)

    for c in a_copies(3):
        c.start()
    stats(15)
    for c in a_copies(4):
        c.start()

    def square_more(s0):
        wait_bytes(gring.at[pl.ds(0, 4)], wsem.at[s0 // 4])
        for t in range(s0, s0 + 4):
            w_square(t)

    square_more(4)
    pack(0)
    a_wait(2)
    square_more(8)
    for t in (8, 9, 10, 11):
        finish(t)
    pack(1)
    square_more(12)
    a_wait(3)
    a_wait(4)
    for t in (12, 13, 14, 15):
        finish(t)
    pack(2)
    for t in range(LAST):
        update(t)
    bs[...] = gather_b(2)
    wait_bytes(attbuf.at[pl.ds(0, NA - 1)], send_sem.at[0])
    wait_bytes(embbuf.at[pl.ds(0, NE - 1)], send_sem.at[1])
    wait_bytes(bbuf.at[:, pl.ds(0, NA * NE - 1)], send_sem.at[2])


def update_body(
    n_total, wn, g3, w3, rq, cq, ro, co, bs, hyper,
    w_qkv_new, w_out_new, rq_new, cq_new, ro_new, co_new,
    obuf, hp, osem, rsem, hsem,
):
    load_hp = pltpu.make_async_copy(hyper, hp, hsem)
    load_hp.start()

    first = []
    for s in range(LAST):
        l, m = place(s)
        first.append(pltpu.make_async_copy(wn.at[s], w_qkv_new.at[l, m], osem.at[0]))
        first[-1].start()
    small = [
        pltpu.make_async_copy(rq, rq_new, rsem.at[0]),
        pltpu.make_async_copy(cq, cq_new, rsem.at[1]),
        pltpu.make_async_copy(ro, ro_new, rsem.at[2]),
        pltpu.make_async_copy(co, co_new, rsem.at[3]),
    ]
    for c in small:
        c.start()
    load_hp.wait()
    step = step_sizes(bs[...], n_total, hp[1], hp[2])
    sl = [pl.ds(c * LANES, LANES) for c in range(4)]
    last = []
    for l in range(LAYERS):
        rows, cols = [ro[l : l + 1, i] for i in sl], [co[l : l + 1, i] for i in sl]
        update_one(obuf.at[l], w3.at[l], g3.at[l], rows, cols, step[:, l : l + 1])
        last.append(pltpu.make_async_copy(obuf.at[l], w_out_new.at[l], osem.at[1 + l]))
        last[-1].start()
    pltpu.make_async_copy(w_qkv_new, w_qkv_new, osem.at[0]).wait()
    for c in last + small:
        c.wait()


def solution(mesh):
    in_specs = (
        P(None, None, "emb", "att"),
        P(None, "att", "emb"),
        P(None, None, "emb"),
        P(None, None, None, "att"),
        P(None, None, "att"),
        P(None, None, "emb"),
        P(None, None, "emb"),
        P(None, None, "att"),
        P(None, "att"),
        P(None, "emb"),
        P(),
    )
    out_specs = (
        P(None, None, "emb", "att"),
        P(None, "att", "emb"),
        P(None, None, "emb"),
        P(None, None, "att"),
        P(None, "att"),
        P(None, "emb"),
    )
    n_total = B * NA
    hbm = pl.BlockSpec(memory_space=pltpu.HBM)
    vm = pl.BlockSpec(memory_space=pltpu.VMEM)
    dma = pltpu.SemaphoreType.DMA

    def local_run(w_qkv, w_out, x_in, dy_qkv, x_attn, dy_out, r_qkv, c_qkv, r_out, c_out, hyper_params):
        ng = len(GROUPS)
        swap = lambda v: jnp.transpose(v, (1, 0, 2))
        mid = pl.pallas_call(
            functools.partial(stats_body, n_total),
            out_shape=(
                pltpu.VMEM((LAST, B, B), F32),
                pltpu.VMEM((4, B, B), F32),
                pltpu.VMEM((4, B, B), F32),
                pltpu.VMEM((3, LAYERS, B), F32),
                pltpu.VMEM((3, LAYERS, B), F32),
                pltpu.VMEM((LAYERS, B), F32),
                pltpu.VMEM((LAYERS, B), F32),
                pltpu.VMEM((1, LANES), F32),
            ),
            in_specs=[hbm] * 11,
            out_specs=(vm,) * 8,
            scratch_shapes=[
                pltpu.VMEM((NX, TOK, B), BF16),
                pltpu.VMEM((NDY, TOK, B), BF16),
                pltpu.VMEM((NA, MATS, 4, LANES), F32),
                pltpu.VMEM((NE, MATS, 4, LANES), F32),
                pltpu.VMEM((len(TILES), NA * NE, 1, LANES), F32),
                pltpu.VMEM((3, LAYERS, B), F32),
                pltpu.VMEM((3, LAYERS, B), F32),
                pltpu.VMEM((LAYERS, B), F32),
                pltpu.VMEM((LAYERS, B), F32),
                pltpu.SMEM((3,), F32),
                pltpu.VMEM((NG, B, B), F32),
                dma((NX,)),
                dma((NDY,)),
                dma((NW,)),
                dma((5,)),
                dma((KCH,)),
                dma((3,)),
                dma((ng,)),
                dma((ng,)),
                dma((len(TILES),)),
            ],
            compiler_params=pltpu.CompilerParams(
                collective_id=0, has_side_effects=True, vmem_limit_bytes=42 * 2**20
            ),
            name="stats",
        )(w_qkv, w_out, x_in, dy_qkv, x_attn, dy_out, swap(r_qkv), swap(c_qkv), r_out, c_out, hyper_params)
        new = pl.pallas_call(
            functools.partial(update_body, n_total),
            out_shape=(
                jax.ShapeDtypeStruct(w_qkv.shape, F32),
                jax.ShapeDtypeStruct(w_out.shape, F32),
                jax.ShapeDtypeStruct((3, LAYERS, B), F32),
                jax.ShapeDtypeStruct((3, LAYERS, B), F32),
                jax.ShapeDtypeStruct(r_out.shape, F32),
                jax.ShapeDtypeStruct(c_out.shape, F32),
            ),
            in_specs=[vm] * 8 + [hbm],
            out_specs=(hbm,) * 6,
            scratch_shapes=[
                pltpu.VMEM((4, B, B), F32),
                pltpu.SMEM((3,), F32),
                dma((1 + LAYERS,)),
                dma((4,)),
                dma,
            ],
            compiler_params=pltpu.CompilerParams(vmem_limit_bytes=6 * 2**20),
            name="update",
        )(*mid, hyper_params)
        return new[0], new[1], swap(new[2]), swap(new[3]), new[4], new[5]

    return jax.shard_map(local_run, mesh=mesh, in_specs=in_specs, out_specs=out_specs, check_vma=False)
```
